32 devices in a mesh: cuts: 2 (over x), wide: 8 (over z, y), batch: 2 (over core).
Axes of the slice: x: 2, y: 2, z: 4, core: 2. Of those that a mesh axis runs over, the one named last changes fastest.
Arguments:
- initial: bfloat16 [2, 64, 2, 2, 256, 256], P('batch', 'cuts', None, None, None, 'wide'), parts along dimension 1, may hold values from -6 to 6
- branches: bfloat16 [8, 2, 2, 256, 2, 256], P(None, None, None, 'batch'), may hold values from -0.1875 to 0.1875
- projectors: float32 [8, 2, 2, 2], replicated, may hold values from -4 to 4
- bits: int32 [2, 8], P('batch'), may hold values from 0 to 1
Outputs:
- amplitudes: float32 [2, 64, 2, 2, 256, 256], P('batch', 'cuts', None, None, 'wide'), parts along dimension 1
The draws below stay inside these ranges and needn't reach their ends.
There are 2 independent parts, one for each index of `cuts`. The reference program is written for one: setup_inputs(seed, part) draws one part's arguments, and reference() takes and returns one part's arrays. A program takes and returns all parts, laid end to end along the dimension named above; an argument that names none is the same for every part. Nothing has to cross between parts.
Inputs may be any that keep to these rules, and one draw needn't show every extreme that they name: `bits`: each entry is a bit.
All inputs are finite; a program needn't handle non-finite values.
Results may differ from the reference program's by a relative error of at most 0.014.
Values may be sent and summed in bfloat16 or wider, within the bound.
A program may use at most 64 MiB of HBM per device.

```python
import jax
import jax.numpy as jnp

QGROUP = 256
HSHARED = 2
COLUMNS = 32
STEPS = 8
BATCH = 2


def set_ends(values, own_key, least, largest):
    dims = values.shape
    place = [jax.random.randint(jax.random.fold_in(own_key, axis), (), 0, dims[axis]) for axis in range(len(dims))]
    values = values.at[tuple(place)].set(least)
    longest = dims.index(max(dims))
    place[longest] = (place[longest] + 1) % dims[longest]
    return values.at[tuple(place)].set(largest)


def level_of(rng, extent, split, smallest, top_value):
    factor_of, own = 1.0, jax.random.fold_in(rng, 6)
    for dim, shards_of in split:
        steps = jnp.exp(jax.random.uniform(jax.random.fold_in(own, dim), (shards_of,), jnp.float32, smallest / len(split), top_value / len(split)))
        factor_of = factor_of * jnp.repeat(steps, extent[dim] // shards_of).reshape([-1 if axis == dim else 1 for axis in range(len(extent))])
    return factor_of


def scatter_about(rng, dims, deviation, limit, pieces=(), kind=jnp.bfloat16):
    values = jax.random.normal(rng, dims, jnp.float32) * deviation
    if len(pieces) > 0:
        values = level_of(rng, dims, pieces, -0.22, 0.18) * values
    return jnp.clip(values, min=-limit, max=limit).astype(kind)


def setup_inputs(seed: int = 0, part: int = 0) -> dict:
    keys = jax.random.split(jax.random.key(seed), 5)
    part_keys = jax.random.split(jax.random.fold_in(keys[4], part), 5)
    initial = scatter_about(part_keys[0], (BATCH, COLUMNS, 2, HSHARED, QGROUP, QGROUP), 1.0, 6.0, ((0, 2), (5, 8)))
    branches = scatter_about(keys[1], (STEPS, 2, HSHARED, QGROUP, HSHARED, QGROUP), (2 * HSHARED * QGROUP) ** -0.5, 0.1875, ((3, 2),))
    projectors = scatter_about(keys[2], (STEPS, 2, 2, HSHARED), 0.7, 4.0, (), jnp.float32)
    bits = set_ends(jax.random.randint(keys[3], (BATCH, STEPS), 0, 2), jax.random.fold_in(keys[3], 1), 0, 1).astype(jnp.int32)
    return {"initial": initial, "branches": branches, "projectors": projectors, "bits": bits}


def contract(state, branch, select):
    prod = jnp.einsum('ncphuv,thugw->ncptgvw', state.astype(jnp.float32), branch.astype(jnp.float32))
    real_part = prod[:, :, 0, 0] - prod[:, :, 1, 1]
    imag_part = prod[:, :, 0, 1] + prod[:, :, 1, 0]
    proj_re = select[:, 0][:, None, :, None, None]
    proj_im = select[:, 1][:, None, :, None, None]
    out_re = proj_re * real_part - proj_im * imag_part
    out_im = proj_re * imag_part + proj_im * real_part
    return jnp.stack([out_re, out_im], axis=2)


def reference(initial, branches, projectors, bits):
    state = initial
    result = None
    for step in range(STEPS):
        chosen = (bits[:, step] == 1)[:, None, None]
        select = jnp.where(chosen, projectors[step, 1][None], projectors[step, 0][None])
        result = contract(state, branches[step], select)
        state = result.astype(jnp.bfloat16)
    return result
```

```python
import functools

import jax
import jax.numpy as jnp
from jax import lax
from jax.experimental import pallas as pl
from jax.experimental.pallas import tpu as pltpu
from jax.sharding import PartitionSpec as P

MESH = pl.DeviceIdType.MESH
F32 = jnp.float32
BF16 = jnp.bfloat16
SIDE = 2


def dot(a, b, dims):
    return lax.dot_general(a, b, (dims, ((), ())), preferred_element_type=F32)


def kernel(wide, pair, x_ref, g_ref, proj_hbm, bits_hbm, out_ref,
           proj_ref, bits_ref, xs, raw, branch, recv1, send2, recv2, state,
           c_sem, x_sem, out_sem, g_send, g_recv, g_local,
           s1_sem, r1_sem, l1_sem, s2_sem, r2_sem, l2_sem, side_sem, know_sem):
    me = lax.axis_index("wide")
    core = lax.axis_index("batch")
    steps = branch.shape[0]
    cols = recv1.shape[0]
    half = g_ref.shape[3]
    group = branch.shape[4]
    vch, width = recv1.shape[4], recv1.shape[5]

    rows = wide // SIDE
    mid = rows // 2
    row, lane = me // SIDE, me % SIDE
    low = row < mid
    inward = jnp.where(low, 1, -1)
    n_in = jnp.where(low, rows - 1 - row, row)
    n_out = rows - 1 - n_in
    middle = n_out == mid - 1

    def device(r, l):
        return r * SIDE + l

    def signal(sem, dev):
        pl.semaphore_signal(sem, inc=1, device_id={"wide": dev}, device_id_type=MESH)

    early = 1

    pieces = [(0, early)] + ([(early, cols - early)] if cols > early else [])

    def stage(i):
        part = pl.ds(*pieces[i])
        return pltpu.make_async_copy(x_ref.at[:, part], xs.at[:, part], x_sem.at[i])

    consts = [pltpu.make_async_copy(proj_hbm, proj_ref, c_sem.at[0]),
              pltpu.make_async_copy(bits_hbm, bits_ref, c_sem.at[1])]

    barrier = pltpu.get_barrier_semaphore()

    @pl.when(middle)
    def _():
        signal(barrier, device(row + inward, lane))

    @pl.when(n_out > 0)
    def _():
        signal(barrier, device(row - inward, lane))

    signal(barrier, device(row, 1 - lane))
    for k in range(1, pair):
        pl.semaphore_signal(barrier, inc=1, device_id={"batch": lax.rem(core + k, pair)}, device_id_type=MESH)
    for i in range(len(pieces)):
        stage(i).start()
    for c in consts:
        c.start()

    def first(j, peer):
        return pltpu.make_async_remote_copy(
            xs.at[peer, j], recv1.at[j, me], s1_sem.at[j, peer], r1_sem.at[j, me],
            device_id={"wide": peer}, device_id_type=MESH)

    def first_from(j, peer):
        return pltpu.make_async_remote_copy(
            xs.at[peer, j], recv1.at[j, peer], s1_sem.at[j, peer], r1_sem.at[j, peer],
            device_id={"wide": peer}, device_id_type=MESH)

    def first_own(j):
        return pltpu.make_async_copy(x_ref.at[me, j], recv1.at[j, me], l1_sem.at[j])

    def second(j, peer):
        return pltpu.make_async_remote_copy(
            send2.at[j, peer], recv2.at[j, me], s2_sem.at[j, peer], r2_sem.at[j, me],
            device_id={"wide": peer}, device_id_type=MESH)

    def second_from(j, peer):
        return pltpu.make_async_remote_copy(
            send2.at[j, peer], recv2.at[j, peer], s2_sem.at[j, peer], r2_sem.at[j, peer],
            device_id={"wide": peer}, device_id_type=MESH)

    def second_own(j):
        return pltpu.make_async_copy(send2.at[j, me], recv2.at[j, me], l2_sem.at[j])

    def mine(s):
        return raw.at[s, :, :, pl.ds(pl.multiple_of(core * half, half), half)]

    def share(s, k):
        return pltpu.make_async_remote_copy(
            g_ref.at[s], mine(s), g_send.at[s, k], g_recv.at[s, k],
            device_id={"batch": lax.rem(core + k, pair)}, device_id_type=MESH)

    def keep(s):
        return pltpu.make_async_copy(g_ref.at[s], mine(s), g_local.at[s])

    def ordered():
        base = jnp.where(low, 0, mid)
        peers = [device(row, 1 - lane)]
        for i in range(1, mid):
            r = base + lax.rem(row - base + i, mid)
            peers += [device(r, lane), device(r, 1 - lane)]
        for i in range(mid):
            r = jnp.where(low, rows - 1 - i, i)
            peers += [device(r, lane), device(r, 1 - lane)]
        return peers

    peers = ordered()

    def first_to(peer, start, stop):
        for j in range(start, stop):
            first(j, peer).start()

    pl.semaphore_wait(barrier, pair + 1)
    signal(side_sem, device(row, 1 - lane))

    @pl.when(jnp.logical_not(middle))
    def _():
        signal(know_sem.at[0, 0], device(row + inward, lane))

    stage(0).wait()
    first_to(device(row + inward, lane), 0, early)
    first_to(device(row, 1 - lane), 0, early)

    def send_branch(s, carry):
        keep(s).start()
        for k in range(1, pair):
            share(s, k).start()
        return carry

    lax.fori_loop(0, steps, send_branch, 0)
    for j in range(cols):
        first_own(j).start()

    pl.semaphore_wait(side_sem, 1)
    first_to(device(row + inward, 1 - lane), 0, early)

    @pl.when(n_out > 0)
    def _():
        pl.semaphore_wait(know_sem.at[0, 0], 1)

        @pl.when(n_in > 0)
        def _():
            signal(know_sem.at[1, 1], device(row - inward, lane))
            for l in range(SIDE):
                first_to(device(row - inward, l), 0, early)

    def tell_in(d):
        @pl.when(middle)
        def _():
            signal(know_sem.at[1, d], device(row + inward, lane))

        @pl.when(jnp.logical_not(middle))
        def _():
            signal(know_sem.at[0, d], device(row + inward, lane))

    @pl.when(n_out > 0)
    def _():
        tell_in(1)

    for d in range(2, rows):
        @pl.when(n_in >= d)
        def _():
            pl.semaphore_wait(know_sem.at[1, d - 1], 1)

            @pl.when(n_out > 0)
            def _():
                signal(know_sem.at[1, d], device(row - inward, lane))
            for l in range(SIDE):
                first_to(device(row + d * inward, l), 0, early)

        @pl.when(n_out >= d)
        def _():
            pl.semaphore_wait(know_sem.at[0, d - 1], 1)
            tell_in(d)
            for l in range(SIDE):
                first_to(device(row - d * inward, l), 0, early)

    for i in range(1, len(pieces)):
        stage(i).wait()
    for j in range(early, cols):
        for p in peers:
            first(j, p).start()

    for c in consts:
        c.wait()

    def arrive(s, carry):
        keep(s).wait()
        for k in range(1, pair):
            share(s, k).wait_recv()
        for p in range(2):
            for h in range(2):
                both = raw[s, p, h]
                for g in range(2):
                    branch[s, p, g, h] = both[:, g, :]
        return carry
    lax.fori_loop(0, steps, arrive, 0)

    def select(s, g):
        hit = bits_ref[0, s] == 1
        return (jnp.where(hit, proj_ref[4 + g, s], proj_ref[g, s]),
                jnp.where(hit, proj_ref[6 + g, s], proj_ref[2 + g, s]))

    def apply(s, lhs, form, put):
        for g in range(2):
            weight = [branch[s, p, g].reshape(2 * group, width) for p in range(2)]
            if form == "flip":
                prod = [[dot(weight[t], lhs[p], ((0,), (0,))) for t in range(2)] for p in range(2)]
            else:
                axis = 1 if form == "rows" else 0
                prod = [[dot(lhs[p], weight[t], ((axis,), (0,))) for t in range(2)] for p in range(2)]
            re = prod[0][0] - prod[1][1]
            im = prod[0][1] + prod[1][0]
            sr, si = select(s, g)
            put(0, g, sr * re - si * im)
            put(1, g, sr * im + si * re)

    def gathered(buf, j):
        return [jnp.concatenate([buf[j, :, p, h].reshape(wide * vch, width) for h in range(2)], axis=1)
                for p in range(2)]

    def gathered_part(buf, j, start, count):
        part = pl.ds(start, count)
        return [jnp.concatenate([buf[j, part, p, h].reshape(count * vch, width) for h in range(2)], axis=1)
                for p in range(2)]

    def held(slot):
        return [state[slot, p].reshape(2 * group, width) for p in range(2)]

    def column(j, carry):
        for p in peers:
            first_from(j, p).wait_recv()
        first_own(j).wait()

        def put_state(slot):
            def put(p, g, value):
                state[slot, p, g] = value.astype(BF16)
            return put

        apply(0, gathered(recv1, j), "rows", put_state(0))

        def middle_step(s, carry):
            apply(s, held((s + 1) % 2), "columns", put_state(s % 2))
            return carry

        lax.fori_loop(1, steps - 2, middle_step, 0)

        def put_send(p, g, value):
            send2[j, :, p, g] = value.astype(BF16).reshape(wide, vch, width)

        apply(steps - 2, held((steps - 3) % 2), "flip", put_send)
        for p in peers:
            second(j, p).start()
        second_own(j).start()
        return carry

    lax.fori_loop(0, cols, column, 0)

    def last(j, carry):
        for p in peers:
            second_from(j, p).wait_recv()
        second_own(j).wait()

        def put_out(p, g, value):
            out_ref[:, j, p, g] = value.reshape(wide, vch, width)

        apply(steps - 1, gathered(recv2, j), "rows", put_out)
        return carry

    lax.fori_loop(0, cols, last, 0)

    def drain(j, carry):
        for p in peers:
            first(j, p).wait_send()
            second(j, p).wait_send()
        return carry

    lax.fori_loop(0, cols, drain, 0)

    def drain_branch(s, carry):
        for k in range(1, pair):
            share(s, k).wait_send()
        return carry

    lax.fori_loop(0, steps, drain_branch, 0)


def solution(mesh):
    wide, pair = mesh.shape["wide"], mesh.shape["batch"]

    def shards(initial, branches, projectors, bits):
        _, columns, parts, shared, group, vch = initial.shape
        steps, half, width = branches.shape[0], branches.shape[3], branches.shape[5]
        cols = columns // wide
        x = jnp.swapaxes(initial, 4, 5).reshape(wide, cols, parts, shared, vch, group)
        proj = jnp.transpose(projectors, (1, 2, 3, 0)).reshape(-1, steps)
        dma = pltpu.SemaphoreType.DMA
        chunk = (cols, wide, parts, shared, vch, width)
        chunk_out = (wide, cols, parts, shared, vch, width)
        out = pl.pallas_call(
            functools.partial(kernel, wide, pair),
            out_shape=jax.ShapeDtypeStruct(chunk_out, F32),
            in_specs=[pl.BlockSpec(memory_space=pltpu.HBM)] * 4,
            out_specs=pl.BlockSpec(memory_space=pltpu.VMEM),
            scratch_shapes=[
                pltpu.SMEM(proj.shape, F32),
                pltpu.SMEM(bits.shape, jnp.int32),
                pltpu.VMEM(x.shape, BF16),
                pltpu.VMEM((steps, parts, shared, half * pair, shared, width), BF16),
                pltpu.VMEM((steps, parts, shared, shared, half * pair, width), BF16),
                pltpu.VMEM(chunk, BF16),
                pltpu.VMEM(chunk, BF16),
                pltpu.VMEM(chunk, BF16),
                pltpu.VMEM((2, parts, shared, group, width), BF16),
                dma((2,)), dma((2,)), dma((cols,)),
                dma((steps, pair)), dma((steps, pair)), dma((steps,)),
                dma((cols, wide)), dma((cols, wide)), dma((cols,)),
                dma((cols, wide)), dma((cols, wide)), dma((cols,)),
                pltpu.SemaphoreType.REGULAR,
                pltpu.SemaphoreType.REGULAR((2, wide // SIDE)),
            ],
            compiler_params=pltpu.CompilerParams(
                collective_id=0, has_side_effects=True, vmem_limit_bytes=44 * 1024 * 1024),
        )(*(pltpu.with_memory_space_constraint(a, pltpu.HBM) for a in (x, branches, proj, bits)))
        return out.reshape(1, columns, parts, shared, vch, width)

    in_specs = (
        P("batch", "cuts", None, None, None, "wide"),
        P(None, None, None, "batch", None, None),
        P(),
        P("batch", None),
    )
    out_specs = P("batch", "cuts", None, None, "wide", None)
    return jax.shard_map(shards, mesh=mesh, in_specs=in_specs, out_specs=out_specs, check_vma=False)
```

```python
import functools
import math

import jax
import jax.numpy as jnp
from jax import lax
from jax.experimental import pallas as pl
from jax.experimental.pallas import tpu as pltpu
from jax.sharding import PartitionSpec as P

MESH = pl.DeviceIdType.MESH
F32 = jnp.float32
BF16 = jnp.bfloat16
SIDE = 2


def dot(a, b, dims):
    return lax.dot_general(a, b, (dims, ((), ())), preferred_element_type=F32)


def kernel(wide, pair, x_ref, g_ref, proj_hbm, bits_hbm, out_ref,
           proj_ref, bits_ref, xs, raw, branch, recv1, send2, recv2, state,
           c_sem, x_sem, g_out, g_in, s1_sem, r1_sem, s2_sem, r2_sem, side_sem, out_know, in_know):
    me = lax.axis_index("wide")
    core = lax.axis_index("batch")
    steps = branch.shape[0]
    cols = recv1.shape[0]
    half = g_ref.shape[3]
    group = branch.shape[4]
    vch, width = recv1.shape[4], recv1.shape[5]

    rows = wide // SIDE
    mid = rows // 2
    row, lane = me // SIDE, me % SIDE
    low = row < mid
    inward = jnp.where(low, 1, -1)
    n_in = jnp.where(low, rows - 1 - row, row)
    n_out = rows - 1 - n_in
    middle = n_out == mid - 1

    def device(r, l):
        return r * SIDE + l

    def signal(sem, dev):
        pl.semaphore_signal(sem, inc=1, device_id={"wide": dev}, device_id_type=MESH)

    def stage(l):
        return pltpu.make_async_copy(x_ref.at[device(row + inward, l), 0], xs.at[l], x_sem)

    consts = [pltpu.make_async_copy(proj_hbm, proj_ref, c_sem.at[0]),
              pltpu.make_async_copy(bits_hbm, bits_ref, c_sem.at[1])]

    barrier = pltpu.get_barrier_semaphore()

    @pl.when(middle)
    def _():
        signal(barrier, device(row + inward, lane))

    @pl.when(n_out > 0)
    def _():
        signal(barrier, device(row - inward, lane))

    signal(barrier, device(row, 1 - lane))
    for k in range(1, pair):
        pl.semaphore_signal(barrier, inc=1, device_id={"batch": lax.rem(core + k, pair)}, device_id_type=MESH)
    for l in range(SIDE):
        stage(l).start()
    for c in consts:
        c.start()

    def filled(ref, sem):
        pltpu.make_async_copy(ref, ref, sem).wait()

    def first(j, peer, src=None):
        return pltpu.make_async_remote_copy(
            x_ref.at[peer, j] if src is None else src, recv1.at[j, me], s1_sem, r1_sem.at[j],
            device_id={"wide": peer}, device_id_type=MESH)

    def first_own(j):
        return pltpu.make_async_copy(x_ref.at[me, j], recv1.at[j, me], r1_sem.at[j])

    def second(j, peer):
        return pltpu.make_async_remote_copy(
            send2.at[j, peer], recv2.at[j, me], s2_sem, r2_sem.at[j],
            device_id={"wide": peer}, device_id_type=MESH)

    batch = steps // g_in.shape[0]

    def mine(s):
        return raw.at[s, :, :, pl.ds(pl.multiple_of(core * half, half), half)]

    def share(s, k):
        return pltpu.make_async_remote_copy(
            g_ref.at[s], mine(s), g_out, g_in.at[s // batch],
            device_id={"batch": lax.rem(core + k, pair)}, device_id_type=MESH)

    def keep(s):
        return pltpu.make_async_copy(g_ref.at[s], mine(s), g_in.at[s // batch])

    def ordered():
        base = jnp.where(low, 0, mid)
        peers = [device(row, 1 - lane)]
        for i in range(1, mid):
            r = base + lax.rem(row - base + i, mid)
            peers += [device(r, lane), device(r, 1 - lane)]
        for i in range(mid):
            r = jnp.where(low, rows - 1 - i, i)
            peers += [device(r, lane), device(r, 1 - lane)]
        return peers

    peers = ordered()

    pl.semaphore_wait(barrier, pair + 1)
    signal(side_sem, device(row, 1 - lane))

    @pl.when(jnp.logical_not(middle))
    def _():
        signal(out_know.at[0], device(row + inward, lane))

    def first_inward(l):
        for i in range(SIDE):
            @pl.when(lane == (i if l == 0 else 1 - i))
            def _():
                first(0, device(row + inward, i), xs.at[i]).start()

    filled(xs, x_sem)
    first_inward(0)
    first(0, device(row, 1 - lane)).start()

    def send_branch(s, carry):
        keep(s).start()
        for k in range(1, pair):
            share(s, k).start()
        return carry

    lax.fori_loop(0, steps, send_branch, 0)
    for j in range(cols):
        first_own(j).start()

    pl.semaphore_wait(side_sem, 1)
    first_inward(1)

    @pl.when(n_out > 0)
    def _():
        pl.semaphore_wait(out_know.at[0], 1)

        @pl.when(n_in > 0)
        def _():
            signal(in_know.at[0], device(row - inward, lane))
            for l in range(SIDE):
                first(0, device(row - inward, l)).start()

    def tell_in(d):
        @pl.when(middle)
        def _():
            signal(in_know.at[d - 1], device(row + inward, lane))

        if d < mid - 1:
            @pl.when(jnp.logical_not(middle))
            def _():
                signal(out_know.at[d], device(row + inward, lane))

    @pl.when(n_out > 0)
    def _():
        tell_in(1)

    for d in range(2, rows):
        @pl.when(n_in >= d)
        def _():
            pl.semaphore_wait(in_know.at[d - 2], 1)
            if d < rows - 1:
                @pl.when(n_out > 0)
                def _():
                    signal(in_know.at[d - 1], device(row - inward, lane))
            for l in range(SIDE):
                first(0, device(row + d * inward, l)).start()

        if d < mid:
            @pl.when(n_out >= d)
            def _():
                pl.semaphore_wait(out_know.at[d - 1], 1)
                tell_in(d)
                for l in range(SIDE):
                    first(0, device(row - d * inward, l)).start()

    for j in range(1, cols):
        for p in peers:
            first(j, p).start()

    for c in consts:
        c.wait()

    def arrive(s, carry):
        @pl.when(lax.rem(s, batch) == 0)
        def _():
            filled(raw.at[pl.ds(s, batch)], g_in.at[s // batch])
        for p in range(2):
            for h in range(2):
                both = raw[s, p, h]
                for g in range(2):
                    branch[s, p, g, h] = both[:, g, :]
        return carry
    lax.fori_loop(0, steps, arrive, 0)

    def select(s, g):
        hit = bits_ref[0, s] == 1
        return (jnp.where(hit, proj_ref[4 + g, s], proj_ref[g, s]),
                jnp.where(hit, proj_ref[6 + g, s], proj_ref[2 + g, s]))

    def apply(s, lhs, form, put):
        for g in range(2):
            weight = [branch[s, p, g].reshape(2 * group, width) for p in range(2)]
            if form == "flip":
                prod = [[dot(weight[t], lhs[p], ((0,), (0,))) for t in range(2)] for p in range(2)]
            else:
                axis = 1 if form == "rows" else 0
                prod = [[dot(lhs[p], weight[t], ((axis,), (0,))) for t in range(2)] for p in range(2)]
            re = prod[0][0] - prod[1][1]
            im = prod[0][1] + prod[1][0]
            sr, si = select(s, g)
            put(0, g, sr * re - si * im)
            put(1, g, sr * im + si * re)

    def gathered(buf, j):
        return [jnp.concatenate([buf[j, :, p, h].reshape(wide * vch, width) for h in range(2)], axis=1)
                for p in range(2)]

    def gathered_part(buf, j, start, count):
        part = pl.ds(start, count)
        return [jnp.concatenate([buf[j, part, p, h].reshape(count * vch, width) for h in range(2)], axis=1)
                for p in range(2)]

    def held(slot):
        return [state[slot, p].reshape(2 * group, width) for p in range(2)]

    def column(j, carry):
        filled(recv1.at[j], r1_sem.at[j])

        def put_state(slot):
            def put(p, g, value):
                state[slot, p, g] = value.astype(BF16)
            return put

        apply(0, gathered(recv1, j), "rows", put_state(0))

        def middle_step(s, carry):
            apply(s, held((s + 1) % 2), "columns", put_state(s % 2))
            return carry

        lax.fori_loop(1, steps - 2, middle_step, 0)

        def put_send(p, g, value):
            send2[j, :, p, g] = value.astype(BF16).reshape(wide, vch, width)

        apply(steps - 2, held((steps - 3) % 2), "flip", put_send)
        for p in peers:
            second(j, p).start()
        recv2[j, me] = send2[j, me]
        return carry

    lax.fori_loop(0, cols, column, 0)

    def last(j, carry):
        filled(recv2.at[j, pl.ds(0, wide - 1)], r2_sem.at[j])

        def put_out(p, g, value):
            out_ref[:, j, p, g] = value.reshape(wide, vch, width)

        apply(steps - 1, gathered(recv2, j), "rows", put_out)
        return carry

    lax.fori_loop(0, cols, last, 0)

    filled(send2.at[:, pl.ds(0, wide - 1)], s1_sem)
    filled(send2.at[:, pl.ds(0, wide - 1)], s2_sem)
    for k in range(1, pair):
        filled(raw.at[:, :, :, pl.ds(0, half)], g_out)


def solution(mesh):
    wide, pair = mesh.shape["wide"], mesh.shape["batch"]

    def shards(initial, branches, projectors, bits):
        _, columns, parts, shared, group, vch = initial.shape
        steps, half, width = branches.shape[0], branches.shape[3], branches.shape[5]
        cols = columns // wide
        x = jnp.swapaxes(initial, 4, 5).reshape(wide, cols, parts, shared, vch, group)
        proj = jnp.transpose(projectors, (1, 2, 3, 0)).reshape(-1, steps)
        dma = pltpu.SemaphoreType.DMA
        chunk = (cols, wide, parts, shared, vch, width)
        chunk_out = (wide, cols, parts, shared, vch, width)
        out = pl.pallas_call(
            functools.partial(kernel, wide, pair),
            out_shape=jax.ShapeDtypeStruct(chunk_out, F32),
            in_specs=[pl.BlockSpec(memory_space=pltpu.HBM)] * 4,
            out_specs=pl.BlockSpec(memory_space=pltpu.VMEM),
            scratch_shapes=[
                pltpu.SMEM(proj.shape, F32),
                pltpu.SMEM(bits.shape, jnp.int32),
                pltpu.VMEM((SIDE,) + x.shape[2:], BF16),
                pltpu.VMEM((steps, parts, shared, half * pair, shared, width), BF16),
                pltpu.VMEM((steps, parts, shared, shared, half * pair, width), BF16),
                pltpu.VMEM(chunk, BF16),
                pltpu.VMEM(chunk, BF16),
                pltpu.VMEM(chunk, BF16),
                pltpu.VMEM((2, parts, shared, group, width), BF16),
                dma((2,)), dma(()), dma(()), dma((math.gcd(2, steps),)),
                dma(()), dma((cols,)), dma(()), dma((cols,)),
                pltpu.SemaphoreType.REGULAR,
                pltpu.SemaphoreType.REGULAR((wide // SIDE // 2 - 1,)),
                pltpu.SemaphoreType.REGULAR((wide // SIDE - 2,)),
            ],
            compiler_params=pltpu.CompilerParams(
                collective_id=0, has_side_effects=True, vmem_limit_bytes=44 * 1024 * 1024),
        )(*(pltpu.with_memory_space_constraint(a, pltpu.HBM) for a in (x, branches, proj, bits)))
        return out.reshape(1, columns, parts, shared, vch, width)

    in_specs = (
        P("batch", "cuts", None, None, None, "wide"),
        P(None, None, None, "batch", None, None),
        P(),
        P("batch", None),
    )
    out_specs = P("batch", "cuts", None, None, "wide", None)
    return jax.shard_map(shards, mesh=mesh, in_specs=in_specs, out_specs=out_specs, check_vma=False)
```

```python
import functools
import math

import jax
import jax.numpy as jnp
from jax import lax
from jax.experimental import pallas as pl
from jax.experimental.pallas import tpu as pltpu
from jax.sharding import PartitionSpec as P

MESH = pl.DeviceIdType.MESH
F32 = jnp.float32
BF16 = jnp.bfloat16
SIDE = 2


def dot(a, b, dims):
    return lax.dot_general(a, b, (dims, ((), ())), preferred_element_type=F32)


def kernel(wide, pair, x_ref, g_ref, proj_hbm, bits_hbm, out_ref,
           proj_ref, bits_ref, xs, raw, branch, recv1, send2, recv2, state,
           c_sem, x_sem, g_out, g_in, s1_sem, r1_sem, s2_sem, r2_sem, side_sem, out_know, in_know):
    me = lax.axis_index("wide")
    core = lax.axis_index("batch")
    steps = branch.shape[0]
    cols = recv1.shape[0]
    half = g_ref.shape[3]
    group = branch.shape[4]
    vch, width = recv1.shape[4], recv1.shape[5]

    rows = wide // SIDE
    mid = rows // 2
    row, lane = me // SIDE, me % SIDE
    low = row < mid
    inward = jnp.where(low, 1, -1)
    n_in = jnp.where(low, rows - 1 - row, row)
    n_out = rows - 1 - n_in
    middle = n_out == mid - 1

    def device(r, l):
        return r * SIDE + l

    def signal(sem, dev):
        pl.semaphore_signal(sem, inc=1, device_id={"wide": dev}, device_id_type=MESH)

    def stage(l):
        return pltpu.make_async_copy(x_ref.at[device(row + inward, l), 0], xs.at[l], x_sem)

    consts = [pltpu.make_async_copy(proj_hbm, proj_ref, c_sem.at[0]),
              pltpu.make_async_copy(bits_hbm, bits_ref, c_sem.at[1])]

    for l in range(SIDE):
        stage(l).start()

    barrier = pltpu.get_barrier_semaphore()

    @pl.when(middle)
    def _():
        signal(barrier, device(row + inward, lane))

    @pl.when(n_out > 0)
    def _():
        signal(barrier, device(row - inward, lane))

    @pl.when(lane == 0)
    def _():
        signal(barrier, device(row, 1))
    for k in range(1, pair):
        pl.semaphore_signal(barrier, inc=1, device_id={"batch": lax.rem(core + k, pair)}, device_id_type=MESH)
    for c in consts:
        c.start()

    def filled(ref, sem):
        pltpu.make_async_copy(ref, ref, sem).wait()

    def first(j, peer, src=None):
        return pltpu.make_async_remote_copy(
            x_ref.at[peer, j] if src is None else src, recv1.at[j, me], s1_sem, r1_sem.at[j],
            device_id={"wide": peer}, device_id_type=MESH)

    def first_own(j):
        return pltpu.make_async_copy(x_ref.at[me, j], recv1.at[j, me], r1_sem.at[j])

    def second(j, peer, arrived):
        return pltpu.make_async_remote_copy(
            send2.at[j, peer], recv2.at[j, me], s2_sem, r2_sem.at[arrived],
            device_id={"wide": peer}, device_id_type=MESH)

    batch = steps // g_in.shape[0]

    def mine(s):
        return raw.at[s, :, :, pl.ds(pl.multiple_of(core * half, half), half)]

    def share(s, k):
        return pltpu.make_async_remote_copy(
            g_ref.at[s], mine(s), g_out, g_in.at[s // batch],
            device_id={"batch": lax.rem(core + k, pair)}, device_id_type=MESH)

    def keep(s):
        return pltpu.make_async_copy(g_ref.at[s], mine(s), g_in.at[s // batch])

    def ordered():
        base = jnp.where(low, 0, mid)
        peers = [device(row, 1 - lane)]
        for i in range(1, mid):
            r = base + lax.rem(row - base + i, mid)
            peers += [device(r, lane), device(r, 1 - lane)]
        for i in range(mid):
            r = jnp.where(low, mid + i, i)
            peers += [device(r, l) for l in range(SIDE)]
        return peers

    peers = ordered()
    near = mid * SIDE - 1

    @pl.when(lane == 0)
    def _():
        pl.semaphore_wait(barrier, pair)

    @pl.when(lane == 1)
    def _():
        pl.semaphore_wait(barrier, pair + 1)
        signal(side_sem, device(row, 0))

    def first_inward(l):
        for i in range(SIDE):
            @pl.when(lane == (i if l == 0 else 1 - i))
            def _():
                first(0, device(row + inward, i), xs.at[i]).start()

    filled(xs, x_sem)
    first_inward(0)
    for j in range(1, min(cols, 2)):
        first(j, device(row + inward, lane)).start()

    def send_branch(s, carry):
        keep(s).start()
        for k in range(1, pair):
            share(s, k).start()
        return carry

    lax.fori_loop(0, steps, send_branch, 0)
    for j in range(cols):
        first_own(j).start()

    pl.semaphore_wait(side_sem, 1)

    @pl.when(lane == 0)
    def _():
        signal(side_sem, device(row, 1))

    @pl.when(jnp.logical_not(middle))
    def _():
        signal(out_know.at[0], device(row + inward, lane))

    first(0, device(row, 1 - lane)).start()
    first_inward(1)

    @pl.when(n_out > 0)
    def _():
        pl.semaphore_wait(out_know.at[0], 1)

        @pl.when(n_in > 0)
        def _():
            signal(in_know.at[0], device(row - inward, lane))
            for l in range(SIDE):
                first(0, device(row - inward, l)).start()

    def tell_in(d):
        @pl.when(middle)
        def _():
            signal(in_know.at[d - 1], device(row + inward, lane))

        if d < mid - 1:
            @pl.when(jnp.logical_not(middle))
            def _():
                signal(out_know.at[d], device(row + inward, lane))

    @pl.when(n_out > 0)
    def _():
        tell_in(1)

    for d in range(2, rows):
        @pl.when(n_in >= d)
        def _():
            pl.semaphore_wait(in_know.at[d - 2], 1)
            if d < rows - 1:
                @pl.when(n_out > 0)
                def _():
                    signal(in_know.at[d - 1], device(row - inward, lane))
            for l in range(SIDE):
                first(0, device(row + d * inward, l)).start()

        if d < mid:
            @pl.when(n_out >= d)
            def _():
                pl.semaphore_wait(out_know.at[d - 1], 1)
                tell_in(d)
                for l in range(SIDE):
                    first(0, device(row - d * inward, l)).start()

    for j in range(1, cols):
        for p in peers:
            if j < 2:
                @pl.when(p != device(row + inward, lane))
                def _():
                    first(j, p).start()
            else:
                first(j, p).start()

    for c in consts:
        c.wait()

    def arrive(s, carry):
        @pl.when(lax.rem(s, batch) == 0)
        def _():
            filled(raw.at[pl.ds(s, batch)], g_in.at[s // batch])
        for p in range(2):
            for h in range(2):
                both = raw[s, p, h]
                for g in range(2):
                    branch[s, p, g, h] = both[:, g, :]
        return carry
    lax.fori_loop(0, steps, arrive, 0)

    def select(s, g):
        hit = bits_ref[0, s] == 1
        return (jnp.where(hit, proj_ref[4 + g, s], proj_ref[g, s]),
                jnp.where(hit, proj_ref[6 + g, s], proj_ref[2 + g, s]))

    def apply(s, lhs, form, put):
        for g in range(2):
            weight = [branch[s, p, g].reshape(2 * group, width) for p in range(2)]
            if form == "flip":
                prod = [[dot(weight[t], lhs[p], ((0,), (0,))) for t in range(2)] for p in range(2)]
            else:
                axis = 1 if form == "rows" else 0
                prod = [[dot(lhs[p], weight[t], ((axis,), (0,))) for t in range(2)] for p in range(2)]
            re = prod[0][0] - prod[1][1]
            im = prod[0][1] + prod[1][0]
            sr, si = select(s, g)
            put(0, g, sr * re - si * im)
            put(1, g, sr * im + si * re)

    def gathered(buf, j, start, count):
        part = pl.ds(start, count)
        return [jnp.concatenate([buf[j, part, p, h].reshape(count * vch, width) for h in range(2)], axis=1)
                for p in range(2)]

    def held(slot):
        return [state[slot, p].reshape(2 * group, width) for p in range(2)]

    def column(j, carry):
        filled(recv1.at[j], r1_sem.at[j])

        def put_state(slot):
            def put(p, g, value):
                state[slot, p, g] = value.astype(BF16)
            return put

        apply(0, gathered(recv1, j, 0, wide), "rows", put_state(0))

        def middle_step(s, carry):
            apply(s, held((s + 1) % 2), "columns", put_state(s % 2))
            return carry

        lax.fori_loop(1, steps - 2, middle_step, 0)

        def put_send(p, g, value):
            send2[j, :, p, g] = value.astype(BF16).reshape(wide, vch, width)

        apply(steps - 2, held((steps - 3) % 2), "flip", put_send)
        final = (j == cols - 1).astype(jnp.int32)
        for i, p in enumerate(peers):
            second(j, p, j + final if i >= near else j).start()
        recv2[j, me] = send2[j, me]
        return carry

    lax.fori_loop(0, cols, column, 0)

    def finish(j, start, count):
        def put_out(p, g, value):
            out_ref[pl.ds(start, count), j, p, g] = value.reshape(count, vch, width)

        apply(steps - 1, gathered(recv2, j, start, count), "rows", put_out)

    def last(j, carry):
        filled(recv2.at[j, pl.ds(0, wide - 1)], r2_sem.at[j])
        finish(j, 0, wide)
        return carry

    lax.fori_loop(0, cols - 1, last, 0)
    here = jnp.where(low, 0, near + 1)
    filled(recv2.at[cols - 1, pl.ds(0, near)], r2_sem.at[cols - 1])
    finish(cols - 1, here, near + 1)
    filled(recv2.at[cols - 1, pl.ds(0, near + 1)], r2_sem.at[cols])
    finish(cols - 1, near + 1 - here, near + 1)

    filled(send2.at[:, pl.ds(0, wide - 1)], s1_sem)
    filled(send2.at[:, pl.ds(0, wide - 1)], s2_sem)
    for k in range(1, pair):
        filled(raw.at[:, :, :, pl.ds(0, half)], g_out)


def solution(mesh):
    wide, pair = mesh.shape["wide"], mesh.shape["batch"]

    def shards(initial, branches, projectors, bits):
        _, columns, parts, shared, group, vch = initial.shape
        steps, half, width = branches.shape[0], branches.shape[3], branches.shape[5]
        cols = columns // wide
        x = jnp.swapaxes(initial, 4, 5).reshape(wide, cols, parts, shared, vch, group)
        proj = jnp.transpose(projectors, (1, 2, 3, 0)).reshape(-1, steps)
        dma = pltpu.SemaphoreType.DMA
        chunk = (cols, wide, parts, shared, vch, width)
        chunk_out = (wide, cols, parts, shared, vch, width)
        out = pl.pallas_call(
            functools.partial(kernel, wide, pair),
            out_shape=jax.ShapeDtypeStruct(chunk_out, F32),
            in_specs=[pl.BlockSpec(memory_space=pltpu.HBM)] * 4,
            out_specs=pl.BlockSpec(memory_space=pltpu.VMEM),
            scratch_shapes=[
                pltpu.SMEM(proj.shape, F32),
                pltpu.SMEM(bits.shape, jnp.int32),
                pltpu.VMEM((SIDE,) + x.shape[2:], BF16),
                pltpu.VMEM((steps, parts, shared, half * pair, shared, width), BF16),
                pltpu.VMEM((steps, parts, shared, shared, half * pair, width), BF16),
                pltpu.VMEM(chunk, BF16),
                pltpu.VMEM(chunk, BF16),
                pltpu.VMEM(chunk, BF16),
                pltpu.VMEM((2, parts, shared, group, width), BF16),
                dma((2,)), dma(()), dma(()), dma((math.gcd(2, steps),)),
                dma(()), dma((cols,)), dma(()), dma((cols + 1,)),
                pltpu.SemaphoreType.REGULAR,
                pltpu.SemaphoreType.REGULAR((wide // SIDE // 2 - 1,)),
                pltpu.SemaphoreType.REGULAR((wide // SIDE - 2,)),
            ],
            compiler_params=pltpu.CompilerParams(
                collective_id=0, has_side_effects=True, vmem_limit_bytes=44 * 1024 * 1024),
        )(*(pltpu.with_memory_space_constraint(a, pltpu.HBM) for a in (x, branches, proj, bits)))
        return out.reshape(1, columns, parts, shared, vch, width)

    in_specs = (
        P("batch", "cuts", None, None, None, "wide"),
        P(None, None, None, "batch", None, None),
        P(),
        P("batch", None),
    )
    out_specs = P("batch", "cuts", None, None, "wide", None)
    return jax.shard_map(shards, mesh=mesh, in_specs=in_specs, out_specs=out_specs, check_vma=False)
```

```python
import functools
import math

import jax
import jax.numpy as jnp
from jax import lax
from jax.experimental import pallas as pl
from jax.experimental.pallas import tpu as pltpu
from jax.sharding import PartitionSpec as P

MESH = pl.DeviceIdType.MESH
F32 = jnp.float32
BF16 = jnp.bfloat16
SIDE = 2


def dot(a, b, dims):
    return lax.dot_general(a, b, (dims, ((), ())), preferred_element_type=F32)


def kernel(wide, pair, x_ref, g_ref, proj_hbm, bits_hbm, out_ref,
           proj_ref, bits_ref, xs, raw, branch, recv1, send2, recv2, state,
           c_sem, x_sem, g_out, g_in, s1_sem, r1_sem, s2_sem, r2_sem, side_sem, out_know, in_know):
    me = lax.axis_index("wide")
    core = lax.axis_index("batch")
    steps = branch.shape[0]
    cols = recv1.shape[0]
    half = g_ref.shape[3]
    group = branch.shape[4]
    vch, width = recv1.shape[4], recv1.shape[5]

    rows = wide // SIDE
    mid = rows // 2
    row, lane = me // SIDE, me % SIDE
    low = row < mid
    inward = jnp.where(low, 1, -1)
    n_in = jnp.where(low, rows - 1 - row, row)
    n_out = rows - 1 - n_in
    middle = n_out == mid - 1

    def device(r, l):
        return r * SIDE + l

    def signal(sem, dev):
        pl.semaphore_signal(sem, inc=1, device_id={"wide": dev}, device_id_type=MESH)

    def stage(l):
        return pltpu.make_async_copy(x_ref.at[device(row + inward, l), 0], xs.at[l], x_sem)

    consts = [pltpu.make_async_copy(proj_hbm, proj_ref, c_sem.at[0]),
              pltpu.make_async_copy(bits_hbm, bits_ref, c_sem.at[1])]

    for l in range(SIDE):
        stage(l).start()

    barrier = pltpu.get_barrier_semaphore()

    @pl.when(middle)
    def _():
        signal(barrier, device(row + inward, lane))

    @pl.when(n_out > 0)
    def _():
        signal(barrier, device(row - inward, lane))

    @pl.when(lane == 0)
    def _():
        signal(barrier, device(row, 1))
    for k in range(1, pair):
        pl.semaphore_signal(barrier, inc=1, device_id={"batch": lax.rem(core + k, pair)}, device_id_type=MESH)
    for c in consts:
        c.start()

    def filled(ref, sem):
        pltpu.make_async_copy(ref, ref, sem).wait()

    def first(j, peer, src=None):
        return pltpu.make_async_remote_copy(
            x_ref.at[peer, j] if src is None else src, recv1.at[j, me], s1_sem, r1_sem.at[j],
            device_id={"wide": peer}, device_id_type=MESH)

    def first_own(j):
        return pltpu.make_async_copy(x_ref.at[me, j], recv1.at[j, me], r1_sem.at[j])

    def second(j, peer, arrived):
        return pltpu.make_async_remote_copy(
            send2.at[j, peer], recv2.at[j, me], s2_sem, r2_sem.at[arrived],
            device_id={"wide": peer}, device_id_type=MESH)

    batch = steps // g_in.shape[0]

    def mine(s):
        return raw.at[s, :, :, pl.ds(pl.multiple_of(core * half, half), half)]

    def share(s, k):
        return pltpu.make_async_remote_copy(
            g_ref.at[s], mine(s), g_out, g_in.at[s // batch],
            device_id={"batch": lax.rem(core + k, pair)}, device_id_type=MESH)

    def keep(s):
        return pltpu.make_async_copy(g_ref.at[s], mine(s), g_in.at[s // batch])

    def ordered():
        base = jnp.where(low, 0, mid)
        peers = [device(row, 1 - lane)]
        for i in range(1, mid):
            r = base + lax.rem(row - base + i, mid)
            peers += [device(r, lane), device(r, 1 - lane)]
        for i in range(mid):
            r = jnp.where(low, mid + i, i)
            peers += [device(r, l) for l in range(SIDE)]
        return peers

    peers = ordered()
    near = mid * SIDE - 1

    @pl.when(lane == 0)
    def _():
        pl.semaphore_wait(barrier, pair)

    @pl.when(lane == 1)
    def _():
        pl.semaphore_wait(barrier, pair + 1)
        signal(side_sem, device(row, 0))

    def first_inward(l):
        for i in range(SIDE):
            @pl.when(lane == (i if l == 0 else 1 - i))
            def _():
                first(0, device(row + inward, i), xs.at[i]).start()

    filled(xs, x_sem)
    first_inward(0)
    for j in range(1, min(cols, 2)):
        first(j, device(row + inward, lane)).start()

    def send_branch(s, carry):
        keep(s).start()
        for k in range(1, pair):
            share(s, k).start()
        return carry

    lax.fori_loop(0, steps, send_branch, 0)
    for j in range(cols):
        first_own(j).start()

    pl.semaphore_wait(side_sem, 1)

    @pl.when(lane == 0)
    def _():
        signal(side_sem, device(row, 1))

    @pl.when(jnp.logical_not(middle))
    def _():
        signal(out_know.at[0], device(row + inward, lane))

    first(0, device(row, 1 - lane)).start()
    first_inward(1)

    @pl.when(n_out > 0)
    def _():
        pl.semaphore_wait(out_know.at[0], 1)

        @pl.when(n_in > 0)
        def _():
            signal(in_know.at[0], device(row - inward, lane))
            for l in range(SIDE):
                first(0, device(row - inward, l)).start()

    def tell_in(d):
        @pl.when(middle)
        def _():
            signal(in_know.at[d - 1], device(row + inward, lane))

        if d < mid - 1:
            @pl.when(jnp.logical_not(middle))
            def _():
                signal(out_know.at[d], device(row + inward, lane))

    @pl.when(n_out > 0)
    def _():
        tell_in(1)

    for d in range(2, rows):
        @pl.when(n_in >= d)
        def _():
            pl.semaphore_wait(in_know.at[d - 2], 1)
            if d < rows - 1:
                @pl.when(n_out > 0)
                def _():
                    signal(in_know.at[d - 1], device(row - inward, lane))
            for l in range(SIDE):
                first(0, device(row + d * inward, l)).start()

        if d < mid:
            @pl.when(n_out >= d)
            def _():
                pl.semaphore_wait(out_know.at[d - 1], 1)
                tell_in(d)
                for l in range(SIDE):
                    first(0, device(row - d * inward, l)).start()

    for j in range(1, cols):
        for p in peers:
            if j < 2:
                @pl.when(p != device(row + inward, lane))
                def _():
                    first(j, p).start()
            else:
                first(j, p).start()

    for c in consts:
        c.wait()

    def arrive(s, carry):
        @pl.when(lax.rem(s, batch) == 0)
        def _():
            filled(raw.at[pl.ds(s, batch)], g_in.at[s // batch])
        for p in range(2):
            for h in range(2):
                both = raw[s, p, h]
                for g in range(2):
                    branch[s, p, g, h] = both[:, g, :]
        return carry
    lax.fori_loop(0, steps, arrive, 0)

    def select(s, g):
        hit = bits_ref[0, s] == 1
        return (jnp.where(hit, proj_ref[4 + g, s], proj_ref[g, s]),
                jnp.where(hit, proj_ref[6 + g, s], proj_ref[2 + g, s]))

    def apply(s, lhs, form, put):
        for g in range(2):
            weight = [branch[s, p, g].reshape(2 * group, width) for p in range(2)]
            if form == "flip":
                prod = [[dot(weight[t], lhs[p], ((0,), (0,))) for t in range(2)] for p in range(2)]
            else:
                axis = 1 if form == "rows" else 0
                prod = [[dot(lhs[p], weight[t], ((axis,), (0,))) for t in range(2)] for p in range(2)]
            re = prod[0][0] - prod[1][1]
            im = prod[0][1] + prod[1][0]
            sr, si = select(s, g)
            put(0, g, sr * re - si * im)
            put(1, g, sr * im + si * re)

    def gathered(buf, j, start, count):
        part = pl.ds(start, count)
        return [jnp.concatenate([buf[j, part, p, h].reshape(count * vch, width) for h in range(2)], axis=1)
                for p in range(2)]

    def held(slot):
        return [state[slot, p].reshape(2 * group, width) for p in range(2)]

    def column(j, carry):
        filled(recv1.at[j], r1_sem.at[j])

        def put_state(slot):
            def put(p, g, value):
                state[slot, p, g] = value.astype(BF16)
            return put

        apply(0, gathered(recv1, j, 0, wide), "rows", put_state(0))

        def middle_step(s, carry):
            apply(s, held((s + 1) % 2), "columns", put_state(s % 2))
            return carry

        lax.fori_loop(1, steps - 2, middle_step, 0)

        def put_send(p, g, value):
            send2[j, :, p, g] = value.astype(BF16).reshape(wide, vch, width)

        apply(steps - 2, held((steps - 3) % 2), "flip", put_send)
        for p in peers[:near]:
            second(j, p, j).start()
        across = peers[near:]
        split = len(across) // 2 if cols > 1 else len(across)

        @pl.when(j < cols - 2)
        def _():
            for p in across:
                second(j, p, j).start()

        if cols > 1:
            @pl.when(j == cols - 2)
            def _():
                for p in across[:split]:
                    second(j, p, j).start()

        @pl.when(j == cols - 1)
        def _():
            second(j, across[0], cols).start()
            for p in across[split:-1]:
                second(j - 1, p, j - 1).start()
            for p in across[1:-1]:
                second(j, p, cols).start()
            for p in across[split:][-1:]:
                second(j - 1, p, j - 1).start()
            second(j, across[-1], cols).start()

        recv2[j, me] = send2[j, me]
        return carry

    lax.fori_loop(0, cols, column, 0)

    def finish(j, start, count):
        def put_out(p, g, value):
            out_ref[pl.ds(start, count), j, p, g] = value.reshape(count, vch, width)

        apply(steps - 1, gathered(recv2, j, start, count), "rows", put_out)

    def last(j, carry):
        filled(recv2.at[j, pl.ds(0, wide - 1)], r2_sem.at[j])
        finish(j, 0, wide)
        return carry

    here = jnp.where(low, 0, near + 1)

    def finish_near():
        filled(recv2.at[cols - 1, pl.ds(0, near)], r2_sem.at[cols - 1])
        finish(cols - 1, here, near + 1)

    def last_and_near(j, carry):
        @pl.when(j == cols - 2)
        def _():
            finish_near()
        return last(j, carry)

    lax.fori_loop(0, cols - 1, last_and_near, 0)
    if cols == 1:
        finish_near()
    filled(recv2.at[cols - 1, pl.ds(0, near + 1)], r2_sem.at[cols])
    finish(cols - 1, near + 1 - here, near + 1)

    filled(send2.at[:, pl.ds(0, wide - 1)], s1_sem)
    filled(send2.at[:, pl.ds(0, wide - 1)], s2_sem)
    for k in range(1, pair):
        filled(raw.at[:, :, :, pl.ds(0, half)], g_out)


def solution(mesh):
    wide, pair = mesh.shape["wide"], mesh.shape["batch"]

    def shards(initial, branches, projectors, bits):
        _, columns, parts, shared, group, vch = initial.shape
        steps, half, width = branches.shape[0], branches.shape[3], branches.shape[5]
        cols = columns // wide
        x = jnp.swapaxes(initial, 4, 5).reshape(wide, cols, parts, shared, vch, group)
        proj = jnp.transpose(projectors, (1, 2, 3, 0)).reshape(-1, steps)
        dma = pltpu.SemaphoreType.DMA
        chunk = (cols, wide, parts, shared, vch, width)
        chunk_out = (wide, cols, parts, shared, vch, width)
        out = pl.pallas_call(
            functools.partial(kernel, wide, pair),
            out_shape=jax.ShapeDtypeStruct(chunk_out, F32),
            in_specs=[pl.BlockSpec(memory_space=pltpu.HBM)] * 4,
            out_specs=pl.BlockSpec(memory_space=pltpu.VMEM),
            scratch_shapes=[
                pltpu.SMEM(proj.shape, F32),
                pltpu.SMEM(bits.shape, jnp.int32),
                pltpu.VMEM((SIDE,) + x.shape[2:], BF16),
                pltpu.VMEM((steps, parts, shared, half * pair, shared, width), BF16),
                pltpu.VMEM((steps, parts, shared, shared, half * pair, width), BF16),
                pltpu.VMEM(chunk, BF16),
                pltpu.VMEM(chunk, BF16),
                pltpu.VMEM(chunk, BF16),
                pltpu.VMEM((2, parts, shared, group, width), BF16),
                dma((2,)), dma(()), dma(()), dma((math.gcd(2, steps),)),
                dma(()), dma((cols,)), dma(()), dma((cols + 1,)),
                pltpu.SemaphoreType.REGULAR,
                pltpu.SemaphoreType.REGULAR((wide // SIDE // 2 - 1,)),
                pltpu.SemaphoreType.REGULAR((wide // SIDE - 2,)),
            ],
            compiler_params=pltpu.CompilerParams(
                collective_id=0, has_side_effects=True, vmem_limit_bytes=44 * 1024 * 1024),
        )(*(pltpu.with_memory_space_constraint(a, pltpu.HBM) for a in (x, branches, proj, bits)))
        return out.reshape(1, columns, parts, shared, vch, width)

    in_specs = (
        P("batch", "cuts", None, None, None, "wide"),
        P(None, None, None, "batch", None, None),
        P(),
        P("batch", None),
    )
    out_specs = P("batch", "cuts", None, None, "wide", None)
    return jax.shard_map(shards, mesh=mesh, in_specs=in_specs, out_specs=out_specs, check_vma=False)
```

```python
import functools
import math

import jax
import jax.numpy as jnp
from jax import lax
from jax.experimental import pallas as pl
from jax.experimental.pallas import tpu as pltpu
from jax.sharding import PartitionSpec as P

MESH = pl.DeviceIdType.MESH
F32 = jnp.float32
BF16 = jnp.bfloat16
SIDE = 2


def dot(a, b, dims):
    return lax.dot_general(a, b, (dims, ((), ())), preferred_element_type=F32)


def scaled(prod, sr, si, put):
    re = prod[0][0] - prod[1][1]
    im = prod[0][1] + prod[1][0]
    put(0, value=sr * re - si * im)
    put(1, value=sr * im + si * re)


def finish_late(wide, done_ref, late_ref, weight_ref, scale_ref, out_ref, result, sem, late_sem):
    cols, count = done_ref.shape[1], late_ref.shape[0]
    vch, width = late_ref.shape[3], late_ref.shape[4]
    here = jnp.where(lax.axis_index("wide") < count, 0, count)
    there = count - here

    def whole(j):
        return pltpu.make_async_copy(done_ref.at[:, j], out_ref.at[:, j], sem.at[j])

    def mine():
        part = pl.ds(here, count)
        return pltpu.make_async_copy(done_ref.at[part, cols - 1], out_ref.at[part, cols - 1], sem.at[cols - 1])

    def late():
        return pltpu.make_async_copy(result, out_ref.at[pl.ds(there, count), cols - 1], late_sem)

    for j in range(cols - 1):
        whole(j).start()
    mine().start()
    lhs = [jnp.concatenate([late_ref[:, p, h].reshape(count * vch, width) for h in range(2)], axis=1)
           for p in range(2)]
    for g in range(2):
        weight = [weight_ref[p, g].reshape(-1, width) for p in range(2)]
        prod = [[dot(lhs[p], weight[t], ((1,), (0,))) for t in range(2)] for p in range(2)]

        def put(p, value):
            result[:, p, g] = value.reshape(count, vch, width)

        scaled(prod, scale_ref[g, 0], scale_ref[g, 1], put)
    late().start()
    for j in range(cols - 1):
        whole(j).wait()
    mine().wait()
    late().wait()


def kernel(wide, pair, x_ref, g_ref, proj_hbm, bits_hbm, out_ref, late_ref, weight_ref, scale_ref,
           proj_ref, bits_ref, xs, raw, branch, recv1, send2, recv2, state,
           c_sem, x_sem, g_out, g_in, s1_sem, r1_sem, s2_sem, r2_sem, side_sem, out_know, in_know):
    me = lax.axis_index("wide")
    core = lax.axis_index("batch")
    steps = branch.shape[0]
    cols = recv1.shape[0]
    half = g_ref.shape[3]
    group = branch.shape[4]
    vch, width = recv1.shape[4], recv1.shape[5]

    rows = wide // SIDE
    mid = rows // 2
    row, lane = me // SIDE, me % SIDE
    low = row < mid
    inward = jnp.where(low, 1, -1)
    n_in = jnp.where(low, rows - 1 - row, row)
    n_out = rows - 1 - n_in
    middle = n_out == mid - 1

    def device(r, l):
        return r * SIDE + l

    def signal(sem, dev):
        pl.semaphore_signal(sem, inc=1, device_id={"wide": dev}, device_id_type=MESH)

    def stage(l):
        return pltpu.make_async_copy(x_ref.at[device(row + inward, l), 0], xs.at[l], x_sem)

    consts = [pltpu.make_async_copy(proj_hbm, proj_ref, c_sem.at[0]),
              pltpu.make_async_copy(bits_hbm, bits_ref, c_sem.at[1])]

    for l in range(SIDE):
        stage(l).start()

    barrier = pltpu.get_barrier_semaphore()

    @pl.when(middle)
    def _():
        signal(barrier, device(row + inward, lane))

    @pl.when(n_out > 0)
    def _():
        signal(barrier, device(row - inward, lane))

    @pl.when(lane == 0)
    def _():
        signal(barrier, device(row, 1))
    for k in range(1, pair):
        pl.semaphore_signal(barrier, inc=1, device_id={"batch": lax.rem(core + k, pair)}, device_id_type=MESH)
    for c in consts:
        c.start()

    def filled(ref, sem):
        pltpu.make_async_copy(ref, ref, sem).wait()

    def first(j, peer, src=None):
        return pltpu.make_async_remote_copy(
            x_ref.at[peer, j] if src is None else src, recv1.at[j, me], s1_sem, r1_sem.at[j],
            device_id={"wide": peer}, device_id_type=MESH)

    def first_own(j):
        return pltpu.make_async_copy(x_ref.at[me, j], recv1.at[j, me], r1_sem.at[j])

    def second(j, peer, arrived):
        return pltpu.make_async_remote_copy(
            send2.at[j, peer], recv2.at[j, me], s2_sem, r2_sem.at[arrived],
            device_id={"wide": peer}, device_id_type=MESH)

    batch = steps // g_in.shape[0]

    def mine(s):
        return raw.at[s, :, :, pl.ds(pl.multiple_of(core * half, half), half)]

    def share(s, k):
        return pltpu.make_async_remote_copy(
            g_ref.at[s], mine(s), g_out, g_in.at[s // batch],
            device_id={"batch": lax.rem(core + k, pair)}, device_id_type=MESH)

    def keep(s):
        return pltpu.make_async_copy(g_ref.at[s], mine(s), g_in.at[s // batch])

    def ordered():
        base = jnp.where(low, 0, mid)
        peers = [device(row, 1 - lane)]
        for i in range(1, mid):
            r = base + lax.rem(row - base + i, mid)
            peers += [device(r, lane), device(r, 1 - lane)]
        for i in range(mid):
            r = jnp.where(low, mid + i, i)
            peers += [device(r, l) for l in range(SIDE)]
        return peers

    peers = ordered()
    near = mid * SIDE - 1

    @pl.when(lane == 0)
    def _():
        pl.semaphore_wait(barrier, pair)

    @pl.when(lane == 1)
    def _():
        pl.semaphore_wait(barrier, pair + 1)
        signal(side_sem, device(row, 0))

    def first_inward(l):
        for i in range(SIDE):
            @pl.when(lane == (i if l == 0 else 1 - i))
            def _():
                first(0, device(row + inward, i), xs.at[i]).start()

    filled(xs, x_sem)
    first_inward(0)
    for j in range(1, min(cols, 2)):
        first(j, device(row + inward, lane)).start()

    def send_branch(s, carry):
        keep(s).start()
        for k in range(1, pair):
            share(s, k).start()
        return carry

    lax.fori_loop(0, steps, send_branch, 0)
    for j in range(cols):
        first_own(j).start()

    pl.semaphore_wait(side_sem, 1)

    @pl.when(lane == 0)
    def _():
        signal(side_sem, device(row, 1))

    @pl.when(jnp.logical_not(middle))
    def _():
        signal(out_know.at[0], device(row + inward, lane))

    first(0, device(row, 1 - lane)).start()
    first_inward(1)

    @pl.when(n_out > 0)
    def _():
        pl.semaphore_wait(out_know.at[0], 1)

        @pl.when(n_in > 0)
        def _():
            signal(in_know.at[0], device(row - inward, lane))
            for l in range(SIDE):
                first(0, device(row - inward, l)).start()

    def tell_in(d):
        @pl.when(middle)
        def _():
            signal(in_know.at[d - 1], device(row + inward, lane))

        if d < mid - 1:
            @pl.when(jnp.logical_not(middle))
            def _():
                signal(out_know.at[d], device(row + inward, lane))

    @pl.when(n_out > 0)
    def _():
        tell_in(1)

    for d in range(2, rows):
        @pl.when(n_in >= d)
        def _():
            pl.semaphore_wait(in_know.at[d - 2], 1)
            if d < rows - 1:
                @pl.when(n_out > 0)
                def _():
                    signal(in_know.at[d - 1], device(row - inward, lane))
            for l in range(SIDE):
                first(0, device(row + d * inward, l)).start()

        if d < mid:
            @pl.when(n_out >= d)
            def _():
                pl.semaphore_wait(out_know.at[d - 1], 1)
                tell_in(d)
                for l in range(SIDE):
                    first(0, device(row - d * inward, l)).start()

    for j in range(1, cols):
        for p in peers:
            if j < 2:
                @pl.when(p != device(row + inward, lane))
                def _():
                    first(j, p).start()
            else:
                first(j, p).start()

    for c in consts:
        c.wait()

    def arrive(s, carry):
        @pl.when(lax.rem(s, batch) == 0)
        def _():
            filled(raw.at[pl.ds(s, batch)], g_in.at[s // batch])
        for p in range(2):
            for h in range(2):
                both = raw[s, p, h]
                for g in range(2):
                    branch[s, p, g, h] = both[:, g, :]
        return carry
    lax.fori_loop(0, steps, arrive, 0)

    def select(s, g):
        hit = bits_ref[0, s] == 1
        return (jnp.where(hit, proj_ref[4 + g, s], proj_ref[g, s]),
                jnp.where(hit, proj_ref[6 + g, s], proj_ref[2 + g, s]))

    def apply(s, lhs, form, put):
        for g in range(2):
            weight = [branch[s, p, g].reshape(2 * group, width) for p in range(2)]
            if form == "flip":
                prod = [[dot(weight[t], lhs[p], ((0,), (0,))) for t in range(2)] for p in range(2)]
            else:
                axis = 1 if form == "rows" else 0
                prod = [[dot(lhs[p], weight[t], ((axis,), (0,))) for t in range(2)] for p in range(2)]
            scaled(prod, *select(s, g), functools.partial(put, g=g))

    def gathered(buf, j, start, count):
        part = pl.ds(start, count)
        return [jnp.concatenate([buf[j, part, p, h].reshape(count * vch, width) for h in range(2)], axis=1)
                for p in range(2)]

    def held(slot):
        return [state[slot, p].reshape(2 * group, width) for p in range(2)]

    def column(j, carry):
        filled(recv1.at[j], r1_sem.at[j])

        def put_state(slot):
            def put(p, g, value):
                state[slot, p, g] = value.astype(BF16)
            return put

        apply(0, gathered(recv1, j, 0, wide), "rows", put_state(0))

        def middle_step(s, carry):
            apply(s, held((s + 1) % 2), "columns", put_state(s % 2))
            return carry

        lax.fori_loop(1, steps - 2, middle_step, 0)

        def put_send(p, g, value):
            send2[j, :, p, g] = value.astype(BF16).reshape(wide, vch, width)

        apply(steps - 2, held((steps - 3) % 2), "flip", put_send)
        for p in peers[:near]:
            second(j, p, j).start()
        across = peers[near:]
        split = len(across) // 2 if cols > 1 else len(across)

        @pl.when(j < cols - 2)
        def _():
            for p in across:
                second(j, p, j).start()

        if cols > 1:
            @pl.when(j == cols - 2)
            def _():
                for p in across[:split]:
                    second(j, p, j).start()

        @pl.when(j == cols - 1)
        def _():
            second(j, across[0], cols).start()
            for p in across[split:-1]:
                second(j - 1, p, j - 1).start()
            for p in across[1:-1]:
                second(j, p, cols).start()
            for p in across[split:][-1:]:
                second(j - 1, p, j - 1).start()
            second(j, across[-1], cols).start()

        recv2[j, me] = send2[j, me]
        return carry

    lax.fori_loop(0, cols, column, 0)

    def finish(j, start, count):
        def put_out(p, g, value):
            out_ref[pl.ds(start, count), j, p, g] = value.reshape(count, vch, width)

        apply(steps - 1, gathered(recv2, j, start, count), "rows", put_out)

    def last(j, carry):
        filled(recv2.at[j, pl.ds(0, wide - 1)], r2_sem.at[j])
        finish(j, 0, wide)
        return carry

    here = jnp.where(low, 0, near + 1)

    def finish_near():
        filled(recv2.at[cols - 1, pl.ds(0, near)], r2_sem.at[cols - 1])
        finish(cols - 1, here, near + 1)

    def last_and_near(j, carry):
        @pl.when(j == cols - 2)
        def _():
            finish_near()
        return last(j, carry)

    lax.fori_loop(0, cols - 1, last_and_near, 0)
    if cols == 1:
        finish_near()
    weight_ref[...] = branch[steps - 1]
    for g in range(2):
        for i, value in enumerate(select(steps - 1, g)):
            scale_ref[g, i] = jnp.full(scale_ref.shape[2:], value, F32)
    filled(recv2.at[cols - 1, pl.ds(0, near + 1)], r2_sem.at[cols])
    late_ref[...] = recv2[cols - 1, pl.ds(near + 1 - here, near + 1)]

    filled(send2.at[:, pl.ds(0, wide - 1)], s1_sem)
    filled(send2.at[:, pl.ds(0, wide - 1)], s2_sem)
    for k in range(1, pair):
        filled(raw.at[:, :, :, pl.ds(0, half)], g_out)


def solution(mesh):
    wide, pair = mesh.shape["wide"], mesh.shape["batch"]

    def shards(initial, branches, projectors, bits):
        _, columns, parts, shared, group, vch = initial.shape
        steps, half, width = branches.shape[0], branches.shape[3], branches.shape[5]
        cols = columns // wide
        x = jnp.swapaxes(initial, 4, 5).reshape(wide, cols, parts, shared, vch, group)
        proj = jnp.transpose(projectors, (1, 2, 3, 0)).reshape(-1, steps)
        dma = pltpu.SemaphoreType.DMA
        chunk = (cols, wide, parts, shared, vch, width)
        chunk_out = (wide, cols, parts, shared, vch, width)
        late = (wide // 2, parts, shared, vch, width)
        last = (parts, shared, shared, half * pair, width)
        ends = pl.pallas_call(
            functools.partial(kernel, wide, pair),
            out_shape=[jax.ShapeDtypeStruct(chunk_out, F32), jax.ShapeDtypeStruct(late, BF16),
                       jax.ShapeDtypeStruct(last, BF16), jax.ShapeDtypeStruct((2, 2, 1, width), F32)],
            in_specs=[pl.BlockSpec(memory_space=pltpu.HBM)] * 4,
            out_specs=[pl.BlockSpec(memory_space=pltpu.VMEM)] * 4,
            scratch_shapes=[
                pltpu.SMEM(proj.shape, F32),
                pltpu.SMEM(bits.shape, jnp.int32),
                pltpu.VMEM((SIDE,) + x.shape[2:], BF16),
                pltpu.VMEM((steps, parts, shared, half * pair, shared, width), BF16),
                pltpu.VMEM((steps, parts, shared, shared, half * pair, width), BF16),
                pltpu.VMEM(chunk, BF16),
                pltpu.VMEM(chunk, BF16),
                pltpu.VMEM(chunk, BF16),
                pltpu.VMEM((2, parts, shared, group, width), BF16),
                dma((2,)), dma(()), dma(()), dma((math.gcd(2, steps),)),
                dma(()), dma((cols,)), dma(()), dma((cols + 1,)),
                pltpu.SemaphoreType.REGULAR,
                pltpu.SemaphoreType.REGULAR((wide // SIDE // 2 - 1,)),
                pltpu.SemaphoreType.REGULAR((wide // SIDE - 2,)),
            ],
            compiler_params=pltpu.CompilerParams(
                collective_id=0, has_side_effects=True, vmem_limit_bytes=44 * 1024 * 1024),
        )(*(pltpu.with_memory_space_constraint(a, pltpu.HBM) for a in (x, branches, proj, bits)))
        out = pl.pallas_call(
            functools.partial(finish_late, wide),
            out_shape=jax.ShapeDtypeStruct(chunk_out, F32),
            in_specs=[pl.BlockSpec(memory_space=pltpu.VMEM)] * 4,
            out_specs=pl.BlockSpec(memory_space=pltpu.HBM),
            scratch_shapes=[pltpu.VMEM((wide // 2, parts, shared, vch, width), F32), dma((cols,)), dma(())],
            compiler_params=pltpu.CompilerParams(vmem_limit_bytes=16 * 1024 * 1024),
        )(*(pltpu.with_memory_space_constraint(a, pltpu.VMEM) for a in ends))
        return out.reshape(1, columns, parts, shared, vch, width)

    in_specs = (
        P("batch", "cuts", None, None, None, "wide"),
        P(None, None, None, "batch", None, None),
        P(),
        P("batch", None),
    )
    out_specs = P("batch", "cuts", None, None, "wide", None)
    return jax.shard_map(shards, mesh=mesh, in_specs=in_specs, out_specs=out_specs, check_vma=False)
```

```python
import functools
import math

import jax
import jax.numpy as jnp
from jax import lax
from jax.experimental import pallas as pl
from jax.experimental.pallas import tpu as pltpu
from jax.sharding import PartitionSpec as P

MESH = pl.DeviceIdType.MESH
F32 = jnp.float32
BF16 = jnp.bfloat16
SIDE = 2


def dot(a, b, dims):
    return lax.dot_general(a, b, (dims, ((), ())), preferred_element_type=F32)


def scaled(prod, sr, si, put):
    re = prod[0][0] - prod[1][1]
    im = prod[0][1] + prod[1][0]
    put(0, value=sr * re - si * im)
    put(1, value=sr * im + si * re)


def finish_late(wide, done_ref, late_ref, weight_ref, scale_ref, out_ref, result, sem, late_sem):
    cols, count = done_ref.shape[1], late_ref.shape[0]
    vch, width = late_ref.shape[3], late_ref.shape[4]
    here = jnp.where(lax.axis_index("wide") < count, 0, count)
    there = count - here

    def whole(j):
        return pltpu.make_async_copy(done_ref.at[:, j], out_ref.at[:, j], sem.at[j])

    def mine():
        part = pl.ds(here, count)
        return pltpu.make_async_copy(done_ref.at[part, cols - 1], out_ref.at[part, cols - 1], sem.at[cols - 1])

    def late():
        return pltpu.make_async_copy(result, out_ref.at[pl.ds(there, count), cols - 1], late_sem)

    for j in range(cols - 1):
        whole(j).start()
    mine().start()
    lhs = [jnp.concatenate([late_ref[:, p, h].reshape(count * vch, width) for h in range(2)], axis=1)
           for p in range(2)]
    for g in range(2):
        weight = [weight_ref[p, g].reshape(-1, width) for p in range(2)]
        prod = [[dot(lhs[p], weight[t], ((1,), (0,))) for t in range(2)] for p in range(2)]

        def put(p, value):
            result[:, p, g] = value.reshape(count, vch, width)

        scaled(prod, scale_ref[g, 0], scale_ref[g, 1], put)
    late().start()
    for j in range(cols - 1):
        whole(j).wait()
    mine().wait()
    late().wait()


def kernel(wide, pair, x_ref, g_ref, proj_hbm, bits_hbm, out_ref, late_ref, weight_ref, scale_ref,
           proj_ref, bits_ref, xs, raw, branch, recv1, send2, recv2, state,
           c_sem, x_sem, g_out, g_in, s1_sem, r1_sem, s2_sem, r2_sem, side_sem, out_know, in_know):
    me = lax.axis_index("wide")
    core = lax.axis_index("batch")
    steps = branch.shape[0]
    cols = recv1.shape[0]
    half = g_ref.shape[3]
    group = branch.shape[4]
    vch, width = recv1.shape[4], recv1.shape[5]

    rows = wide // SIDE
    mid = rows // 2
    row, lane = me // SIDE, me % SIDE
    low = row < mid
    inward = jnp.where(low, 1, -1)
    n_in = jnp.where(low, rows - 1 - row, row)
    n_out = rows - 1 - n_in
    middle = n_out == mid - 1

    def device(r, l):
        return r * SIDE + l

    def signal(sem, dev):
        pl.semaphore_signal(sem, inc=1, device_id={"wide": dev}, device_id_type=MESH)

    def stage(l):
        return pltpu.make_async_copy(x_ref.at[device(row + inward, l), 0], xs.at[l], x_sem)

    consts = [pltpu.make_async_copy(proj_hbm, proj_ref, c_sem.at[0]),
              pltpu.make_async_copy(bits_hbm, bits_ref, c_sem.at[1])]

    for l in range(SIDE):
        stage(l).start()

    barrier = pltpu.get_barrier_semaphore()

    @pl.when(middle)
    def _():
        signal(barrier, device(row + inward, lane))

    @pl.when(n_out > 0)
    def _():
        signal(barrier, device(row - inward, lane))

    @pl.when(lane == 0)
    def _():
        signal(barrier, device(row, 1))
    for k in range(1, pair):
        pl.semaphore_signal(barrier, inc=1, device_id={"batch": lax.rem(core + k, pair)}, device_id_type=MESH)
    for c in consts:
        c.start()

    def filled(ref, sem):
        pltpu.make_async_copy(ref, ref, sem).wait()

    def first(j, peer, src=None):
        return pltpu.make_async_remote_copy(
            x_ref.at[peer, j] if src is None else src, recv1.at[j, me], s1_sem, r1_sem.at[j],
            device_id={"wide": peer}, device_id_type=MESH)

    def first_own(j):
        return pltpu.make_async_copy(x_ref.at[me, j], recv1.at[j, me], r1_sem.at[j])

    def second(j, peer, arrived):
        return pltpu.make_async_remote_copy(
            send2.at[j, peer], recv2.at[j, me], s2_sem, r2_sem.at[arrived],
            device_id={"wide": peer}, device_id_type=MESH)

    batch = steps // g_in.shape[0]

    def mine(s):
        return raw.at[s, :, :, pl.ds(pl.multiple_of(core * half, half), half)]

    def share(s, k):
        return pltpu.make_async_remote_copy(
            g_ref.at[s], mine(s), g_out, g_in.at[s // batch],
            device_id={"batch": lax.rem(core + k, pair)}, device_id_type=MESH)

    def keep(s):
        return pltpu.make_async_copy(g_ref.at[s], mine(s), g_in.at[s // batch])

    def ordered():
        base = jnp.where(low, 0, mid)
        peers = [device(row, 1 - lane)]
        for i in range(1, mid):
            r = base + lax.rem(row - base + i, mid)
            peers += [device(r, lane), device(r, 1 - lane)]
        for i in range(mid):
            r = jnp.where(low, mid + i, i)
            peers += [device(r, l) for l in range(SIDE)]
        return peers

    peers = ordered()
    near = mid * SIDE - 1

    @pl.when(lane == 0)
    def _():
        pl.semaphore_wait(barrier, pair)

    @pl.when(lane == 1)
    def _():
        pl.semaphore_wait(barrier, pair + 1)
        signal(side_sem, device(row, 0))

    def first_inward(l):
        for i in range(SIDE):
            @pl.when(lane == (i if l == 0 else 1 - i))
            def _():
                first(0, device(row + inward, i), xs.at[i]).start()

    filled(xs, x_sem)
    first_inward(0)
    for j in range(1, min(cols, 2)):
        first(j, device(row + inward, lane)).start()

    for j in range(cols):
        first_own(j).start()

    pl.semaphore_wait(side_sem, 1)

    @pl.when(lane == 0)
    def _():
        signal(side_sem, device(row, 1))

    @pl.when(jnp.logical_not(middle))
    def _():
        signal(out_know.at[0], device(row + inward, lane))

    first(0, device(row, 1 - lane)).start()
    first_inward(1)

    @pl.when(n_out > 0)
    def _():
        pl.semaphore_wait(out_know.at[0], 1)

        @pl.when(n_in > 0)
        def _():
            signal(in_know.at[0], device(row - inward, lane))
            for l in range(SIDE):
                first(0, device(row - inward, l)).start()

    def tell_in(d):
        @pl.when(middle)
        def _():
            signal(in_know.at[d - 1], device(row + inward, lane))

        if d < mid - 1:
            @pl.when(jnp.logical_not(middle))
            def _():
                signal(out_know.at[d], device(row + inward, lane))

    @pl.when(n_out > 0)
    def _():
        tell_in(1)

    for d in range(2, rows):
        @pl.when(n_in >= d)
        def _():
            pl.semaphore_wait(in_know.at[d - 2], 1)
            if d < rows - 1:
                @pl.when(n_out > 0)
                def _():
                    signal(in_know.at[d - 1], device(row - inward, lane))
            for l in range(SIDE):
                first(0, device(row + d * inward, l)).start()

        if d < mid:
            @pl.when(n_out >= d)
            def _():
                pl.semaphore_wait(out_know.at[d - 1], 1)
                tell_in(d)
                for l in range(SIDE):
                    first(0, device(row - d * inward, l)).start()

    for j in range(1, cols):
        for p in peers:
            if j < 2:
                @pl.when(p != device(row + inward, lane))
                def _():
                    first(j, p).start()
            else:
                first(j, p).start()

    def send_branch(s, carry):
        keep(s).start()
        for k in range(1, pair):
            share(s, k).start()
        return carry

    lax.fori_loop(0, steps, send_branch, 0)
    for c in consts:
        c.wait()

    def arrive(s, carry):
        @pl.when(lax.rem(s, batch) == 0)
        def _():
            filled(raw.at[pl.ds(s, batch)], g_in.at[s // batch])
        for p in range(2):
            for h in range(2):
                both = raw[s, p, h]
                for g in range(2):
                    branch[s, p, g, h] = both[:, g, :]
        return carry
    lax.fori_loop(0, steps, arrive, 0)

    def select(s, g):
        hit = bits_ref[0, s] == 1
        return (jnp.where(hit, proj_ref[4 + g, s], proj_ref[g, s]),
                jnp.where(hit, proj_ref[6 + g, s], proj_ref[2 + g, s]))

    def apply(s, lhs, form, put):
        for g in range(2):
            weight = [branch[s, p, g].reshape(2 * group, width) for p in range(2)]
            if form == "flip":
                prod = [[dot(weight[t], lhs[p], ((0,), (0,))) for t in range(2)] for p in range(2)]
            else:
                axis = 1 if form == "rows" else 0
                prod = [[dot(lhs[p], weight[t], ((axis,), (0,))) for t in range(2)] for p in range(2)]
            scaled(prod, *select(s, g), functools.partial(put, g=g))

    def gathered(buf, j, start, count):
        part = pl.ds(start, count)
        return [jnp.concatenate([buf[j, part, p, h].reshape(count * vch, width) for h in range(2)], axis=1)
                for p in range(2)]

    def held(slot):
        return [state[slot, p].reshape(2 * group, width) for p in range(2)]

    def column(j, carry):
        filled(recv1.at[j], r1_sem.at[j])

        def put_state(slot):
            def put(p, g, value):
                state[slot, p, g] = value.astype(BF16)
            return put

        apply(0, gathered(recv1, j, 0, wide), "rows", put_state(0))

        def middle_step(s, carry):
            apply(s, held((s + 1) % 2), "columns", put_state(s % 2))
            return carry

        lax.fori_loop(1, steps - 2, middle_step, 0)

        def put_send(p, g, value):
            send2[j, :, p, g] = value.astype(BF16).reshape(wide, vch, width)

        apply(steps - 2, held((steps - 3) % 2), "flip", put_send)
        for p in peers[:near]:
            second(j, p, j).start()
        across = peers[near:]
        split = len(across) // 2 if cols > 1 else len(across)

        @pl.when(j < cols - 2)
        def _():
            for p in across:
                second(j, p, j).start()

        if cols > 1:
            @pl.when(j == cols - 2)
            def _():
                for p in across[:split]:
                    second(j, p, j).start()

        @pl.when(j == cols - 1)
        def _():
            second(j, across[0], cols).start()
            for p in across[split:-1]:
                second(j - 1, p, j - 1).start()
            for p in across[1:-1]:
                second(j, p, cols).start()
            for p in across[split:][-1:]:
                second(j - 1, p, j - 1).start()
            second(j, across[-1], cols).start()

        recv2[j, me] = send2[j, me]
        return carry

    lax.fori_loop(0, cols, column, 0)

    weight_ref[...] = branch[steps - 1]
    for g in range(2):
        for i, value in enumerate(select(steps - 1, g)):
            scale_ref[g, i] = jnp.full(scale_ref.shape[2:], value, F32)

    def finish(j, start, count):
        def put_out(p, g, value):
            out_ref[pl.ds(start, count), j, p, g] = value.reshape(count, vch, width)

        apply(steps - 1, gathered(recv2, j, start, count), "rows", put_out)

    def last(j, carry):
        filled(recv2.at[j, pl.ds(0, wide - 1)], r2_sem.at[j])
        finish(j, 0, wide)
        return carry

    here = jnp.where(low, 0, near + 1)

    def finish_near():
        filled(recv2.at[cols - 1, pl.ds(0, near)], r2_sem.at[cols - 1])
        finish(cols - 1, here, near + 1)

    def last_and_near(j, carry):
        @pl.when(j == cols - 2)
        def _():
            finish_near()
        return last(j, carry)

    lax.fori_loop(0, cols - 1, last_and_near, 0)
    if cols == 1:
        finish_near()
    filled(recv2.at[cols - 1, pl.ds(0, near + 1)], r2_sem.at[cols])
    late_ref[...] = recv2[cols - 1, pl.ds(near + 1 - here, near + 1)]

    filled(send2.at[:, pl.ds(0, wide - 1)], s1_sem)
    filled(send2.at[:, pl.ds(0, wide - 1)], s2_sem)
    for k in range(1, pair):
        filled(raw.at[:, :, :, pl.ds(0, half)], g_out)


def solution(mesh):
    wide, pair = mesh.shape["wide"], mesh.shape["batch"]

    def shards(initial, branches, projectors, bits):
        _, columns, parts, shared, group, vch = initial.shape
        steps, half, width = branches.shape[0], branches.shape[3], branches.shape[5]
        cols = columns // wide
        x = jnp.swapaxes(initial, 4, 5).reshape(wide, cols, parts, shared, vch, group)
        proj = jnp.transpose(projectors, (1, 2, 3, 0)).reshape(-1, steps)
        dma = pltpu.SemaphoreType.DMA
        chunk = (cols, wide, parts, shared, vch, width)
        chunk_out = (wide, cols, parts, shared, vch, width)
        late = (wide // 2, parts, shared, vch, width)
        last = (parts, shared, shared, half * pair, width)
        ends = pl.pallas_call(
            functools.partial(kernel, wide, pair),
            out_shape=[jax.ShapeDtypeStruct(chunk_out, F32), jax.ShapeDtypeStruct(late, BF16),
                       jax.ShapeDtypeStruct(last, BF16), jax.ShapeDtypeStruct((2, 2, 1, width), F32)],
            in_specs=[pl.BlockSpec(memory_space=pltpu.HBM)] * 4,
            out_specs=[pl.BlockSpec(memory_space=pltpu.VMEM)] * 4,
            scratch_shapes=[
                pltpu.SMEM(proj.shape, F32),
                pltpu.SMEM(bits.shape, jnp.int32),
                pltpu.VMEM((SIDE,) + x.shape[2:], BF16),
                pltpu.VMEM((steps, parts, shared, half * pair, shared, width), BF16),
                pltpu.VMEM((steps, parts, shared, shared, half * pair, width), BF16),
                pltpu.VMEM(chunk, BF16),
                pltpu.VMEM(chunk, BF16),
                pltpu.VMEM(chunk, BF16),
                pltpu.VMEM((2, parts, shared, group, width), BF16),
                dma((2,)), dma(()), dma(()), dma((math.gcd(2, steps),)),
                dma(()), dma((cols,)), dma(()), dma((cols + 1,)),
                pltpu.SemaphoreType.REGULAR,
                pltpu.SemaphoreType.REGULAR((wide // SIDE // 2 - 1,)),
                pltpu.SemaphoreType.REGULAR((wide // SIDE - 2,)),
            ],
            compiler_params=pltpu.CompilerParams(
                collective_id=0, has_side_effects=True, vmem_limit_bytes=44 * 1024 * 1024),
        )(*(pltpu.with_memory_space_constraint(a, pltpu.HBM) for a in (x, branches, proj, bits)))
        out = pl.pallas_call(
            functools.partial(finish_late, wide),
            out_shape=jax.ShapeDtypeStruct(chunk_out, F32),
            in_specs=[pl.BlockSpec(memory_space=pltpu.VMEM)] * 4,
            out_specs=pl.BlockSpec(memory_space=pltpu.HBM),
            scratch_shapes=[pltpu.VMEM((wide // 2, parts, shared, vch, width), F32), dma((cols,)), dma(())],
            compiler_params=pltpu.CompilerParams(vmem_limit_bytes=16 * 1024 * 1024),
        )(*(pltpu.with_memory_space_constraint(a, pltpu.VMEM) for a in ends))
        return out.reshape(1, columns, parts, shared, vch, width)

    in_specs = (
        P("batch", "cuts", None, None, None, "wide"),
        P(None, None, None, "batch", None, None),
        P(),
        P("batch", None),
    )
    out_specs = P("batch", "cuts", None, None, "wide", None)
    return jax.shard_map(shards, mesh=mesh, in_specs=in_specs, out_specs=out_specs, check_vma=False)
```

```python
import functools
import math

import jax
import jax.numpy as jnp
from jax import lax
from jax.experimental import pallas as pl
from jax.experimental.pallas import tpu as pltpu
from jax.sharding import PartitionSpec as P

MESH = pl.DeviceIdType.MESH
F32 = jnp.float32
BF16 = jnp.bfloat16
SIDE = 2


def dot(a, b, dims):
    return lax.dot_general(a, b, (dims, ((), ())), preferred_element_type=F32)


def scaled(prod, sr, si, put):
    re = prod[0][0] - prod[1][1]
    im = prod[0][1] + prod[1][0]
    put(0, value=sr * re - si * im)
    put(1, value=sr * im + si * re)


def finish_late(wide, done_ref, late_ref, weight_ref, scale_ref, out_ref, result, sem, late_sem):
    cols, count = done_ref.shape[1], late_ref.shape[0]
    vch, width = late_ref.shape[3], late_ref.shape[4]
    here = jnp.where(lax.axis_index("wide") < count, 0, count)
    there = count - here

    def whole(j):
        return pltpu.make_async_copy(done_ref.at[:, j], out_ref.at[:, j], sem.at[j])

    def mine():
        part = pl.ds(here, count)
        return pltpu.make_async_copy(done_ref.at[part, cols - 1], out_ref.at[part, cols - 1], sem.at[cols - 1])

    def late():
        return pltpu.make_async_copy(result, out_ref.at[pl.ds(there, count), cols - 1], late_sem)

    for j in range(cols - 1):
        whole(j).start()
    mine().start()
    lhs = [jnp.concatenate([late_ref[:, p, h].reshape(count * vch, width) for h in range(2)], axis=1)
           for p in range(2)]
    for g in range(2):
        weight = [weight_ref[p, g].reshape(-1, width) for p in range(2)]
        prod = [[dot(lhs[p], weight[t], ((1,), (0,))) for t in range(2)] for p in range(2)]

        def put(p, value):
            result[:, p, g] = value.reshape(count, vch, width)

        scaled(prod, scale_ref[g, 0], scale_ref[g, 1], put)
    late().start()
    for j in range(cols - 1):
        whole(j).wait()
    mine().wait()
    late().wait()


def kernel(wide, pair, x_ref, g_ref, proj_hbm, bits_hbm, out_ref, late_ref, weight_ref, scale_ref,
           proj_ref, bits_ref, xs, raw, branch, recv1, send2, recv2, state,
           c_sem, x_sem, g_out, g_in, s1_sem, r1_sem, s2_sem, r2_sem, side_sem, out_know, in_know):
    me = lax.axis_index("wide")
    core = lax.axis_index("batch")
    steps = branch.shape[0]
    cols = recv1.shape[0]
    half = g_ref.shape[3]
    group = branch.shape[4]
    vch, width = recv1.shape[4], recv1.shape[5]

    rows = wide // SIDE
    mid = rows // 2
    row, lane = me // SIDE, me % SIDE
    low = row < mid
    inward = jnp.where(low, 1, -1)
    n_in = jnp.where(low, rows - 1 - row, row)
    n_out = rows - 1 - n_in
    middle = n_out == mid - 1

    def device(r, l):
        return r * SIDE + l

    def signal(sem, dev):
        pl.semaphore_signal(sem, inc=1, device_id={"wide": dev}, device_id_type=MESH)

    def stage(l):
        return pltpu.make_async_copy(x_ref.at[device(row + inward, l), 0], xs.at[l], x_sem)

    consts = [pltpu.make_async_copy(proj_hbm, proj_ref, c_sem.at[0]),
              pltpu.make_async_copy(bits_hbm, bits_ref, c_sem.at[1])]

    for l in range(SIDE):
        stage(l).start()

    barrier = pltpu.get_barrier_semaphore()

    @pl.when(middle)
    def _():
        signal(barrier, device(row + inward, lane))

    @pl.when(n_out > 0)
    def _():
        signal(barrier, device(row - inward, lane))

    @pl.when(lane == 0)
    def _():
        signal(barrier, device(row, 1))
    for k in range(1, pair):
        pl.semaphore_signal(barrier, inc=1, device_id={"batch": lax.rem(core + k, pair)}, device_id_type=MESH)
    for c in consts:
        c.start()

    def filled(ref, sem):
        pltpu.make_async_copy(ref, ref, sem).wait()

    def first(j, peer, src=None):
        return pltpu.make_async_remote_copy(
            x_ref.at[peer, j] if src is None else src, recv1.at[j, me], s1_sem, r1_sem.at[j],
            device_id={"wide": peer}, device_id_type=MESH)

    def first_own(j):
        return pltpu.make_async_copy(x_ref.at[me, j], recv1.at[j, me], r1_sem.at[j])

    def second(j, peer, arrived):
        return pltpu.make_async_remote_copy(
            send2.at[j, peer], recv2.at[j, me], s2_sem, r2_sem.at[arrived],
            device_id={"wide": peer}, device_id_type=MESH)

    batch = steps // g_in.shape[0]

    def mine(s):
        return raw.at[s, :, :, pl.ds(pl.multiple_of(core * half, half), half)]

    def share(s, k):
        return pltpu.make_async_remote_copy(
            g_ref.at[s], mine(s), g_out, g_in.at[s // batch],
            device_id={"batch": lax.rem(core + k, pair)}, device_id_type=MESH)

    def keep(s):
        return pltpu.make_async_copy(g_ref.at[s], mine(s), g_in.at[s // batch])

    def ordered():
        base = jnp.where(low, 0, mid)
        peers = [device(row, 1 - lane)]
        for i in range(1, mid):
            r = base + lax.rem(row - base + i, mid)
            peers += [device(r, lane), device(r, 1 - lane)]
        for i in range(mid):
            r = jnp.where(low, mid + i, i)
            peers += [device(r, l) for l in range(SIDE)]
        return peers

    peers = ordered()
    near = mid * SIDE - 1

    @pl.when(lane == 0)
    def _():
        pl.semaphore_wait(barrier, pair)

    @pl.when(lane == 1)
    def _():
        pl.semaphore_wait(barrier, pair + 1)
        signal(side_sem, device(row, 0))

    def first_inward(l):
        for i in range(SIDE):
            @pl.when(lane == (i if l == 0 else 1 - i))
            def _():
                first(0, device(row + inward, i), xs.at[i]).start()

    filled(xs, x_sem)
    first_inward(0)
    for j in range(1, min(cols, 2)):
        first(j, device(row + inward, lane)).start()

    for j in range(cols):
        first_own(j).start()

    pl.semaphore_wait(side_sem, 1)

    @pl.when(lane == 0)
    def _():
        signal(side_sem, device(row, 1))

    @pl.when(jnp.logical_not(middle))
    def _():
        signal(out_know.at[0], device(row + inward, lane))

    first(0, device(row, 1 - lane)).start()
    first_inward(1)

    @pl.when(n_out > 0)
    def _():
        pl.semaphore_wait(out_know.at[0], 1)

        @pl.when(n_in > 0)
        def _():
            signal(in_know.at[0], device(row - inward, lane))
            for l in range(SIDE):
                first(0, device(row - inward, l)).start()

    def tell_in(d):
        @pl.when(middle)
        def _():
            signal(in_know.at[d - 1], device(row + inward, lane))

        if d < mid - 1:
            @pl.when(jnp.logical_not(middle))
            def _():
                signal(out_know.at[d], device(row + inward, lane))

    @pl.when(n_out > 0)
    def _():
        tell_in(1)

    for d in range(2, rows):
        @pl.when(n_in >= d)
        def _():
            pl.semaphore_wait(in_know.at[d - 2], 1)
            if d < rows - 1:
                @pl.when(n_out > 0)
                def _():
                    signal(in_know.at[d - 1], device(row - inward, lane))
            for l in range(SIDE):
                first(0, device(row + d * inward, l)).start()

        if d < mid:
            @pl.when(n_out >= d)
            def _():
                pl.semaphore_wait(out_know.at[d - 1], 1)
                tell_in(d)
                for l in range(SIDE):
                    first(0, device(row - d * inward, l)).start()

    for j in range(1, cols):
        for p in peers:
            if j < 2:
                @pl.when(p != device(row + inward, lane))
                def _():
                    first(j, p).start()
            else:
                first(j, p).start()

    def send_branch(s, carry):
        keep(s).start()
        for k in range(1, pair):
            share(s, k).start()
        return carry

    lax.fori_loop(0, steps, send_branch, 0)
    for c in consts:
        c.wait()

    def arrive(s, carry):
        @pl.when(lax.rem(s, batch) == 0)
        def _():
            filled(raw.at[pl.ds(s, batch)], g_in.at[s // batch])
        for p in range(2):
            for h in range(2):
                both = raw[s, p, h]
                for g in range(2):
                    branch[s, p, g, h] = both[:, g, :]
        return carry
    lax.fori_loop(0, steps, arrive, 0)

    def select(s, g):
        hit = bits_ref[0, s] == 1
        return (jnp.where(hit, proj_ref[4 + g, s], proj_ref[g, s]),
                jnp.where(hit, proj_ref[6 + g, s], proj_ref[2 + g, s]))

    def apply(s, lhs, form, put):
        for g in range(2):
            weight = [branch[s, p, g].reshape(2 * group, width) for p in range(2)]
            if form == "flip":
                prod = [[dot(weight[t], lhs[p], ((0,), (0,))) for t in range(2)] for p in range(2)]
            else:
                axis = 1 if form == "rows" else 0
                prod = [[dot(lhs[p], weight[t], ((axis,), (0,))) for t in range(2)] for p in range(2)]
            scaled(prod, *select(s, g), functools.partial(put, g=g))

    def gathered(buf, j, start, count):
        part = pl.ds(start, count)
        return [jnp.concatenate([buf[j, part, p, h].reshape(count * vch, width) for h in range(2)], axis=1)
                for p in range(2)]

    def held(slot):
        return [state[slot, p].reshape(2 * group, width) for p in range(2)]

    def column(j, carry):
        filled(recv1.at[j], r1_sem.at[j])

        def put_state(slot):
            def put(p, g, value):
                state[slot, p, g] = value.astype(BF16)
            return put

        apply(0, gathered(recv1, j, 0, wide), "rows", put_state(0))

        def middle_step(s, carry):
            apply(s, held((s + 1) % 2), "columns", put_state(s % 2))
            return carry

        lax.fori_loop(1, steps - 2, middle_step, 0)

        def put_send(p, g, value):
            send2[j, :, p, g] = value.astype(BF16).reshape(wide, vch, width)

        apply(steps - 2, held((steps - 3) % 2), "flip", put_send)
        for p in peers[:near]:
            second(j, p, j).start()
        across = peers[near:]
        split = len(across) // 2 if cols > 1 else len(across)

        @pl.when(j < cols - 2)
        def _():
            for p in across:
                second(j, p, j).start()

        if cols > 1:
            @pl.when(j == cols - 2)
            def _():
                for p in across[:split]:
                    second(j, p, j).start()

        @pl.when(j == cols - 1)
        def _():
            second(j, across[0], cols).start()
            for p in across[split:-1]:
                second(j - 1, p, j - 1).start()
            for p in across[1:-1]:
                second(j, p, cols).start()
            for p in across[split:][-1:]:
                second(j - 1, p, j - 1).start()
            second(j, across[-1], cols).start()

        recv2[j, me] = send2[j, me]
        return carry

    lax.fori_loop(0, cols, column, 0)

    filled(send2.at[:, pl.ds(0, wide - 1)], s1_sem)
    for k in range(1, pair):
        filled(raw.at[:, :, :, pl.ds(0, half)], g_out)
    weight_ref[...] = branch[steps - 1]
    for g in range(2):
        for i, value in enumerate(select(steps - 1, g)):
            scale_ref[g, i] = jnp.full(scale_ref.shape[2:], value, F32)

    def finish(j, start, count):
        def put_out(p, g, value):
            out_ref[pl.ds(start, count), j, p, g] = value.reshape(count, vch, width)

        apply(steps - 1, gathered(recv2, j, start, count), "rows", put_out)

    def last(j, carry):
        filled(recv2.at[j, pl.ds(0, wide - 1)], r2_sem.at[j])
        finish(j, 0, wide)
        return carry

    here = jnp.where(low, 0, near + 1)

    def finish_near():
        filled(recv2.at[cols - 1, pl.ds(0, near)], r2_sem.at[cols - 1])
        finish(cols - 1, here, near + 1)

    def last_and_near(j, carry):
        @pl.when(j == cols - 2)
        def _():
            finish_near()
        return last(j, carry)

    lax.fori_loop(0, cols - 1, last_and_near, 0)
    if cols == 1:
        finish_near()
    filled(recv2.at[cols - 1, pl.ds(0, near + 1)], r2_sem.at[cols])
    late_ref[...] = recv2[cols - 1, pl.ds(near + 1 - here, near + 1)]

    filled(send2.at[:, pl.ds(0, wide - 1)], s2_sem)


def solution(mesh):
    wide, pair = mesh.shape["wide"], mesh.shape["batch"]

    def shards(initial, branches, projectors, bits):
        _, columns, parts, shared, group, vch = initial.shape
        steps, half, width = branches.shape[0], branches.shape[3], branches.shape[5]
        cols = columns // wide
        x = jnp.swapaxes(initial, 4, 5).reshape(wide, cols, parts, shared, vch, group)
        proj = jnp.transpose(projectors, (1, 2, 3, 0)).reshape(-1, steps)
        dma = pltpu.SemaphoreType.DMA
        chunk = (cols, wide, parts, shared, vch, width)
        chunk_out = (wide, cols, parts, shared, vch, width)
        late = (wide // 2, parts, shared, vch, width)
        last = (parts, shared, shared, half * pair, width)
        ends = pl.pallas_call(
            functools.partial(kernel, wide, pair),
            out_shape=[jax.ShapeDtypeStruct(chunk_out, F32), jax.ShapeDtypeStruct(late, BF16),
                       jax.ShapeDtypeStruct(last, BF16), jax.ShapeDtypeStruct((2, 2, 1, width), F32)],
            in_specs=[pl.BlockSpec(memory_space=pltpu.HBM)] * 4,
            out_specs=[pl.BlockSpec(memory_space=pltpu.VMEM)] * 4,
            scratch_shapes=[
                pltpu.SMEM(proj.shape, F32),
                pltpu.SMEM(bits.shape, jnp.int32),
                pltpu.VMEM((SIDE,) + x.shape[2:], BF16),
                pltpu.VMEM((steps, parts, shared, half * pair, shared, width), BF16),
                pltpu.VMEM((steps, parts, shared, shared, half * pair, width), BF16),
                pltpu.VMEM(chunk, BF16),
                pltpu.VMEM(chunk, BF16),
                pltpu.VMEM(chunk, BF16),
                pltpu.VMEM((2, parts, shared, group, width), BF16),
                dma((2,)), dma(()), dma(()), dma((math.gcd(2, steps),)),
                dma(()), dma((cols,)), dma(()), dma((cols + 1,)),
                pltpu.SemaphoreType.REGULAR,
                pltpu.SemaphoreType.REGULAR((wide // SIDE // 2 - 1,)),
                pltpu.SemaphoreType.REGULAR((wide // SIDE - 2,)),
            ],
            compiler_params=pltpu.CompilerParams(
                collective_id=0, has_side_effects=True, vmem_limit_bytes=44 * 1024 * 1024),
        )(*(pltpu.with_memory_space_constraint(a, pltpu.HBM) for a in (x, branches, proj, bits)))
        out = pl.pallas_call(
            functools.partial(finish_late, wide),
            out_shape=jax.ShapeDtypeStruct(chunk_out, F32),
            in_specs=[pl.BlockSpec(memory_space=pltpu.VMEM)] * 4,
            out_specs=pl.BlockSpec(memory_space=pltpu.HBM),
            scratch_shapes=[pltpu.VMEM((wide // 2, parts, shared, vch, width), F32), dma((cols,)), dma(())],
            compiler_params=pltpu.CompilerParams(vmem_limit_bytes=16 * 1024 * 1024),
        )(*(pltpu.with_memory_space_constraint(a, pltpu.VMEM) for a in ends))
        return out.reshape(1, columns, parts, shared, vch, width)

    in_specs = (
        P("batch", "cuts", None, None, None, "wide"),
        P(None, None, None, "batch", None, None),
        P(),
        P("batch", None),
    )
    out_specs = P("batch", "cuts", None, None, "wide", None)
    return jax.shard_map(shards, mesh=mesh, in_specs=in_specs, out_specs=out_specs, check_vma=False)
```
